32 devices in a mesh: grp: 4 (over y, core), dp: 8 (over z, x).
Axes of the slice: x: 2, y: 2, z: 4, core: 2. Of those that a mesh axis runs over, the one named last changes fastest.
Arguments:
- tokens: bfloat16 [4, 1024, 2048], P('grp', 'dp'), may hold values from -6 to 6
- hidden_grad: bfloat16 [4, 1024, 6144], P('grp', 'dp'), may hold values from -6 to 6
- w_gate: bfloat16 [4, 2048, 6144], P('grp', None, 'dp'), may hold values from -6 to 6
- w_up: bfloat16 [4, 2048, 6144], P('grp', None, 'dp'), may hold values from -6 to 6
Outputs:
- mixed_gate: bfloat16 [4, 2048, 6144], P('grp', None, 'dp')
- mixed_up: bfloat16 [4, 2048, 6144], P('grp', None, 'dp')
The draws below stay inside these ranges and needn't reach their ends.
All inputs are finite; a program needn't handle non-finite values.
Results may differ from the reference program's by a relative error of at most 0.0052.
Values may be sent and summed in bfloat16 or wider, within the bound.
A program may use at most 256 MiB of HBM per device.

```python
import jax
import jax.numpy as jnp
from jax import lax

D = 2048
FF = 6144
GROUPS = 4
GROUP_TOKENS = 1024


def level_of(rng, shape, cuts, smallest, high):
    def one(axis_at, parts):
        heights = jax.random.uniform(jax.random.fold_in(jax.random.fold_in(rng, 6), axis_at), (parts,), jnp.float32, smallest / len(cuts), high / len(cuts))
        return jnp.repeat(jnp.exp(heights), shape[axis_at] // parts).reshape((-1,) + (1,) * (len(shape) - axis_at - 1))

    loudness = one(*cuts[0])
    for cut in cuts[1:]:
        loudness = loudness * one(*cut)
    return loudness


def scatter_about(key, dims, spread, reach, cuts=(), kind=jnp.bfloat16):
    drawn = jax.random.normal(key, dims, jnp.float32) * spread
    if len(cuts) > 0:
        drawn = level_of(key, dims, cuts, -0.22, 0.18) * drawn
    return jnp.clip(drawn, min=-reach, max=reach).astype(kind)


def setup_inputs(seed: int = 0) -> dict:
    key_of = jax.random.split(jax.random.key(seed), 5)
    tokens = scatter_about(key_of[0], (GROUPS, GROUP_TOKENS, D), 1.0, 6.0, ((0, 4), (1, 8)))
    hidden_grad = scatter_about(key_of[1], (GROUPS, GROUP_TOKENS, FF), 1.0, 6.0, ((0, 4), (1, 8)))
    w_gate = scatter_about(key_of[2], (GROUPS, D, FF), 1.0, 6.0, ((0, 4), (2, 8)))
    w_up = scatter_about(key_of[3], (GROUPS, D, FF), 1.0, 6.0, ((0, 4), (2, 8)))
    return dict(tokens=tokens, hidden_grad=hidden_grad, w_gate=w_gate, w_up=w_up)


def one_replica(operands):
    rows, cotangent, gate_weight, up_weight = operands
    scale = D ** -0.5
    gate = jnp.dot(rows, gate_weight, preferred_element_type=jnp.float32) * scale
    up = jnp.dot(rows, up_weight, preferred_element_type=jnp.float32) * scale
    sigma = jax.nn.sigmoid(gate)
    upstream = cotangent.astype(jnp.float32)
    gate_rows = (upstream * up * sigma * (1.0 + gate * (1.0 - sigma))).astype(jnp.bfloat16)
    up_rows = (upstream * gate * sigma).astype(jnp.bfloat16)
    gate_grad = jnp.dot(rows.T, gate_rows, preferred_element_type=jnp.float32) * scale
    up_grad = jnp.dot(rows.T, up_rows, preferred_element_type=jnp.float32) * scale
    gate_step = (gate_weight.astype(jnp.float32) - 0.5 * gate_grad).astype(jnp.bfloat16)
    up_step = (up_weight.astype(jnp.float32) - 0.5 * up_grad).astype(jnp.bfloat16)
    return gate_step, up_step


def average_cycle(stepped):
    wide = stepped.astype(jnp.float32)
    mixed = 0.5 * wide + 0.25 * (jnp.roll(wide, 1, axis=0) + jnp.roll(wide, -1, axis=0))
    return mixed.astype(jnp.bfloat16)


def reference(tokens, hidden_grad, w_gate, w_up):
    gate_step, up_step = lax.map(one_replica, (tokens, hidden_grad, w_gate, w_up))
    return average_cycle(gate_step), average_cycle(up_step)
```

```python
import functools
import math

import jax
import jax.numpy as jnp
from jax import lax
from jax.experimental import pallas as pl
from jax.experimental.pallas import tpu as pltpu
from jax.sharding import PartitionSpec as P

LANES = 128
BLOCK = 256
VMEM = pl.BlockSpec(memory_space=pltpu.VMEM)
ANY = pl.BlockSpec(memory_space=pl.ANY)
MESH = pl.DeviceIdType.MESH
F32, BF16 = jnp.float32, jnp.bfloat16


def inner_size(n):
    return max(d for d in range(1, n + 1) if n % d == 0 and d * d <= n)


def early_units(units):
    return max(units // 3 // LANES, 1) * LANES


def aligned(index, size):
    return pl.ds(pl.multiple_of(index * size, size), size)


def kernel(n, groups, cut, *refs):
    tokens, hidden, w_gate, w_up, out_gate, out_up = refs[:6]
    tok, tok_t, cot, held, near, far, far_tok, far_tok_t, far_cot, gate_rows, up_rows = refs[6:17]
    local_sem, gather_sems, far_gather_sems, cot_sems, early_sems, early_cot_sems, near_sems, far_sems = (
        refs[17:18] + (refs[18:24], refs[24:30], refs[30:32], refs[32:34], refs[34:36], refs[36:38], refs[38:40])
    )
    nx = inner_size(n)
    nz = n // nx
    rows, depth = tokens.shape
    units = w_gate.shape[1]
    scale = depth ** (-0.5)
    blocks = depth // BLOCK
    grp, me = lax.axis_index("grp"), lax.axis_index("dp")
    z, x = me // nx, lax.rem(me, nx)
    odd = lax.rem(grp, 2) == 1
    near_grp = jnp.where(odd, grp - 1, grp + 1)
    far_grp = jnp.where(odd, lax.rem(grp + 1, groups), lax.rem(grp + groups - 1, groups))

    mine = pltpu.make_async_copy(tokens, tok.at[aligned(me, rows), :], local_sem.at[0])
    mine.start()
    own_cot = pltpu.make_async_copy(
        hidden.at[:, aligned(me, units)], cot.at[aligned(me, rows), :], local_sem.at[1]
    )
    own_cot.start()
    weights = [pltpu.make_async_copy(w, held.at[s], local_sem.at[2 + s]) for s, w in enumerate((w_gate, w_up))]
    for copy in weights:
        copy.start()

    barrier = pltpu.get_barrier_semaphore()
    for j in range(1, n):
        pl.semaphore_signal(barrier, inc=1, device_id={"dp": lax.rem(me + j, n)}, device_id_type=MESH)
    pl.semaphore_signal(barrier, inc=1, device_id={"grp": near_grp}, device_id_type=MESH)
    for j in range(n):
        pl.semaphore_signal(barrier, inc=1, device_id={"grp": far_grp, "dp": j}, device_id_type=MESH)
    pl.semaphore_wait(barrier, 2 * n)

    def remote(src, dst, send, recv, **to):
        return pltpu.make_async_remote_copy(
            src_ref=src, dst_ref=dst, send_sem=send, recv_sem=recv, device_id=to, device_id_type=MESH
        )

    def early_tokens():
        return remote(tokens, far_tok.at[aligned(me, rows), :], early_sems[0].at[0], early_sems[1].at[0], grp=far_grp)

    def early_weights(s):
        return remote(
            (w_gate, w_up)[s].at[:, :cut], far.at[s, :, :cut],
            early_sems[0].at[1 + s], early_sems[1].at[1 + s], grp=far_grp,
        )

    def early_cot(j):
        return remote(
            hidden.at[:, pl.ds(j * units, cut)], far_cot.at[aligned(me, rows), :],
            early_cot_sems[0].at[j], early_cot_sems[1].at[me], grp=far_grp, dp=j,
        )

    def early_cot_arrival(source):
        place = far_cot.at[aligned(source, rows), :]
        return remote(place, place, early_cot_sems[0].at[source], early_cot_sems[1].at[source], grp=far_grp, dp=source)

    @pl.when(odd)
    def _():
        early_tokens().start()
        for s in range(2):
            early_weights(s).start()
        early_weights(0).wait_send()
        for j in range(n):
            early_cot(j).start()
        early_weights(1).wait_send()

    def cot_send(zz, xx):
        to = zz * nx + xx
        return remote(
            hidden.at[:, aligned(to, units)], cot.at[aligned(me, rows), :], cot_sems[0].at[to], cot_sems[1].at[me], dp=to
        )

    def cot_arrival(source):
        place = cot.at[aligned(source, rows), :]
        return remote(place, place, cot_sems[0].at[source], cot_sems[1].at[source], dp=source)

    def collect(buf, turned, cot_buf, weight, gate_out, up_out, sems, send_cot, wait_cot):
        up_send, up_recv, down_send, down_recv, side_send, side_recv = sems

        def slot(zz, xx):
            return buf.at[aligned(zz * nx + xx, rows), :]

        def up(zz):
            return remote(slot(zz, x), slot(zz, x), up_send.at[zz], up_recv.at[zz], dp=(z + 1) * nx + x)

        def up_arrival(zz):
            return remote(slot(zz, x), slot(zz, x), up_send.at[zz], up_recv.at[zz], dp=(z - 1) * nx + x)

        def down(zz):
            return remote(slot(zz, x), slot(zz, x), down_send.at[zz], down_recv.at[zz], dp=(z - 1) * nx + x)

        def down_arrival(zz):
            return remote(slot(zz, x), slot(zz, x), down_send.at[zz], down_recv.at[zz], dp=(z + 1) * nx + x)

        def side(zz, j):
            return remote(
                slot(zz, x), slot(zz, x), side_send.at[zz, j - 1], side_recv.at[zz, j - 1],
                dp=z * nx + lax.rem(x + j, nx),
            )

        def side_arrival(zz, j):
            other = lax.rem(x + nx - j, nx)
            return remote(
                slot(zz, other), slot(zz, other), side_send.at[zz, j - 1], side_recv.at[zz, j - 1], dp=z * nx + other
            )

        def forward_on(zz):
            pl.when(z + 1 < nz)(lambda: up(zz).start())

        def backward_on(zz):
            pl.when(z >= 1)(lambda: down(zz).start())

        forward_on(z)
        backward_on(z)
        for j in range(1, nx):
            side(z, j).start()
        send_cot(0)
        span = nx * rows
        least = jnp.minimum(z, nz - 1 - z)
        longer = jnp.where(z < nz - 1 - z, 1, -1)

        @pl.loop(0, nz)
        def _(r):
            @pl.when((r < nz - 1) & (z - 1 - r >= 0))
            def _():
                zz = z - 1 - r
                up_arrival(zz).wait_recv()
                forward_on(zz)
                for j in range(1, nx):
                    side(zz, j).start()

            @pl.when((r < nz - 1) & (z + 1 + r < nz))
            def _():
                zz = z + 1 + r
                down_arrival(zz).wait_recv()
                backward_on(zz)
                for j in range(1, nx):
                    side(zz, j).start()

            pl.when(r < nz - 1)(lambda: send_cot(r + 1))

            near_turn = r <= 2 * least
            step = jnp.where(near_turn, (r + 1) // 2, r - least)
            sign = jnp.where(near_turn, jnp.where(lax.rem(r, 2) == 1, -1, 1), longer)
            zz = z + sign * step
            for j in range(1, nx):
                side_arrival(zz, j).wait_recv()
            for xx in range(nx):
                wait_cot(zz * nx + xx)
            part = aligned(zz, span)
            block = buf[part, :]
            turned[:, part] = block.T
            gate = jnp.dot(block, weight(0), preferred_element_type=F32) * scale
            up_value = jnp.dot(block, weight(1), preferred_element_type=F32) * scale
            sigma = jax.nn.sigmoid(gate)
            upstream = cot_buf[part, :].astype(F32)
            gate_out(part, (upstream * up_value * sigma * (1.0 + gate * (1.0 - sigma))).astype(BF16))
            up_out(part, (upstream * gate * sigma).astype(BF16))

        def settle():
            @pl.loop(0, nz)
            def _(zz):
                for j in range(1, nx):
                    side(zz, j).wait_send()
                pl.when((z + 1 < nz) & (zz <= z))(lambda: up(zz).wait_send())
                pl.when((z >= 1) & (zz >= z))(lambda: down(zz).wait_send())

        return settle

    def send_cot(d):
        def to_row(zz):
            for xx in range(nx):
                pl.when(zz * nx + xx != me)(lambda: cot_send(zz, xx).start())

        if isinstance(d, int) and d == 0:
            to_row(z)
        else:
            pl.when(z - d >= 0)(lambda: to_row(z - d))
            pl.when(z + d < nz)(lambda: to_row(z + d))

    def wait_cot(source):
        pl.when(source != me)(lambda: cot_arrival(source).wait_recv())

    mine.wait()
    own_cot.wait()
    for copy in weights:
        copy.wait()

    def put(ref, width):
        def store(part, value):
            ref[part, :width] = value

        return store

    settle_own = collect(
        tok, tok_t, cot, lambda s: held[s], put(gate_rows, units), put(up_rows, units), gather_sems, send_cot, wait_cot
    )

    def near_copy(i):
        place = (slice(None), aligned(i, BLOCK), slice(None))
        return remote(held.at[place], near.at[place], near_sems[0].at[i], near_sems[1].at[i], grp=near_grp)

    def far_copy(i, whole):
        place = (slice(None), aligned(i, BLOCK), slice(None) if whole else pl.ds(cut, units - cut))
        return remote(held.at[place], far.at[place], far_sems[0].at[i], far_sems[1].at[i], grp=far_grp)

    def send_steps(i):
        pl.when(odd)(lambda: far_copy(i, False).start())
        pl.when(jnp.logical_not(odd))(lambda: far_copy(i, True).start())
        near_copy(i).start()

    @pl.loop(0, blocks)
    def _(i):
        part = aligned(i, BLOCK)
        turned = tok_t[part, :]
        for s, unit_rows in enumerate((gate_rows, up_rows)):
            gradient = jnp.dot(turned, unit_rows[...], preferred_element_type=F32) * scale
            held[s, part, :] = (held[s, part, :].astype(F32) - 0.5 * gradient).astype(BF16)
        pl.when(i >= 1)(lambda: send_steps(i - 1))

    send_steps(blocks - 1)

    @pl.when(jnp.logical_not(odd))
    def _():
        near_copy(0).wait_recv()
        early_tokens().wait_recv()
        for s in range(2):
            early_weights(s).wait_recv()
        settle_far = collect(
            far_tok, far_tok_t, far_cot, lambda s: far[s, :, :cut], put(gate_rows, cut), put(up_rows, cut),
            far_gather_sems, lambda d: None, lambda source: early_cot_arrival(source).wait_recv(),
        )

        @pl.loop(0, blocks)
        def _(i):
            part = aligned(i, BLOCK)
            turned = far_tok_t[part, :]
            for s, unit_rows in enumerate((gate_rows, up_rows)):
                gradient = jnp.dot(turned, unit_rows[:, :cut], preferred_element_type=F32) * scale
                far[s, part, :cut] = (far[s, part, :cut].astype(F32) - 0.5 * gradient).astype(BF16)

        settle_far()

    @pl.loop(0, blocks)
    def _(i):
        @pl.when(odd)
        def _():
            near_copy(i).wait_recv()
            far_copy(i, True).wait_recv()

        @pl.when(jnp.logical_not(odd))
        def _():
            pl.when(i >= 1)(lambda: near_copy(i).wait_recv())
            far_copy(i, False).wait_recv()

        part = aligned(i, BLOCK)
        for s, out in enumerate((out_gate, out_up)):
            mixed = 0.5 * held[s, part, :].astype(F32) + 0.25 * (
                near[s, part, :].astype(F32) + far[s, part, :].astype(F32)
            )
            out[part, :] = mixed.astype(BF16)

    settle_own()

    @pl.loop(0, n)
    def _(j):
        pl.when(j != me)(lambda: cot_arrival(j).wait_send())

    @pl.when(odd)
    def _():
        early_tokens().wait_send()
        for j in range(n):
            early_cot(j).wait_send()

    @pl.loop(0, blocks)
    def _(i):
        near_copy(i).wait_send()
        pl.when(odd)(lambda: far_copy(i, False).wait_send())
        pl.when(jnp.logical_not(odd))(lambda: far_copy(i, True).wait_send())


def local(tokens, hidden_grad, w_gate, w_up):
    n, groups = lax.axis_size("dp"), lax.axis_size("grp")
    nx = inner_size(n)
    nz = n // nx
    tokens, hidden_grad, w_gate, w_up = tokens[0], hidden_grad[0], w_gate[0], w_up[0]
    rows, depth = tokens.shape
    units = w_gate.shape[1]
    total = n * rows
    cut = early_units(units)
    blocks = depth // BLOCK
    dma = pltpu.SemaphoreType.DMA
    hops = [dma((nz,))] * 4 + [dma((nz, max(nx - 1, 1)))] * 2
    scratch = [
        pltpu.VMEM((total, depth), BF16),
        pltpu.VMEM((depth, total), BF16),
        pltpu.VMEM((total, units), BF16),
        pltpu.VMEM((2, depth, units), BF16),
        pltpu.VMEM((2, depth, units), BF16),
        pltpu.VMEM((2, depth, units), BF16),
        pltpu.VMEM((total, depth), BF16),
        pltpu.VMEM((depth, total), BF16),
        pltpu.VMEM((total, cut), BF16),
        pltpu.VMEM((total, units), BF16),
        pltpu.VMEM((total, units), BF16),
        dma((4,)),
        *hops,
        *hops,
        dma((n,)), dma((n,)),
        dma((3,)), dma((3,)),
        dma((n,)), dma((n,)),
        dma((blocks,)), dma((blocks,)),
        dma((blocks,)), dma((blocks,)),
    ]
    shape = jax.ShapeDtypeStruct(w_gate.shape, w_gate.dtype)
    outs = pl.pallas_call(
        functools.partial(kernel, n, groups, cut),
        out_shape=[shape, shape],
        in_specs=[ANY] * 4,
        out_specs=[VMEM] * 2,
        scratch_shapes=scratch,
        compiler_params=pltpu.CompilerParams(
            collective_id=0, has_side_effects=True, vmem_limit_bytes=56 * 1024 * 1024
        ),
        name="gossip_step",
    )(tokens, hidden_grad, w_gate, w_up)
    return tuple(out[None] for out in outs)


def solution(mesh):
    in_specs = (
        P("grp", "dp", None),
        P("grp", "dp", None),
        P("grp", None, "dp"),
        P("grp", None, "dp"),
    )
    out_specs = (P("grp", None, "dp"), P("grp", None, "dp"))
    return jax.shard_map(local, mesh=mesh, in_specs=in_specs, out_specs=out_specs, check_vma=False)
```

```python
import functools

import jax
import jax.numpy as jnp
from jax import lax
from jax.experimental import pallas as pl
from jax.experimental.pallas import tpu as pltpu
from jax.sharding import PartitionSpec as P

LANES = 128
BLOCK = 256
PIECES = 2
VMEM_LIMIT = 54 * 1024 * 1024
VMEM = pl.BlockSpec(memory_space=pltpu.VMEM)
ANY = pl.BlockSpec(memory_space=pl.ANY)
MESH = pl.DeviceIdType.MESH
F32, BF16 = jnp.float32, jnp.bfloat16


def inner_size(n):
    return max(d for d in range(1, n + 1) if n % d == 0 and d * d <= n)


def slab_count(units):
    return next(count for count in (3, 2, 1) if units % (count * LANES) == 0)


def aligned(index, size):
    return pl.ds(pl.multiple_of(index * size, size), size)


def kernel(n, groups, *refs):
    tokens, hidden, w_gate, w_up, far = refs[:5]
    tok, tok_t, cot, held, near, far_tok, far_tok_t, far_cot, stage, gate_rows, up_rows, gate_pre, up_pre = refs[5:18]
    local_sem, weight_sem, turn_sem = refs[18:21]
    gather_sems, far_gather_sems = refs[21:27], refs[27:33]
    cot_sems, far_cot_sems, early_sems, early_cot_sems, near_sems, far_sems = (
        refs[k : k + 2] for k in range(33, 45, 2)
    )
    nx = inner_size(n)
    nz = n // nx
    rows, depth = tokens.shape
    units = w_gate.shape[1]
    slabs, _, _, width = held.shape
    scale = depth ** (-0.5)
    blocks = depth // BLOCK
    span = nx * rows
    grp, me = lax.axis_index("grp"), lax.axis_index("dp")
    z, x = me // nx, lax.rem(me, nx)
    odd = lax.rem(grp, 2) == 1
    even = jnp.logical_not(odd)
    near_grp = jnp.where(odd, grp - 1, grp + 1)
    far_grp = jnp.where(odd, lax.rem(grp + 1, groups), lax.rem(grp + groups - 1, groups))

    def hidden_part(to, h):
        return hidden.at[:, pl.ds(pl.multiple_of(to * units + h * width, LANES), width)]

    mine = [pltpu.make_async_copy(tokens, tok.at[aligned(me, rows), :], local_sem.at[slabs])]
    for h in range(slabs):
        mine.append(pltpu.make_async_copy(hidden_part(me, h), cot.at[h, aligned(me, rows), :], local_sem.at[h]))
    for h in range(slabs):
        for s, w in enumerate((w_gate, w_up)):
            mine.append(
                pltpu.make_async_copy(w.at[:, pl.ds(h * width, width)], held.at[h, s], weight_sem.at[h, s])
            )
    for copy in mine:
        copy.start()

    with jax.named_scope("barrier"):
        barrier = pltpu.get_barrier_semaphore()

        def greet(**to):
            pl.semaphore_signal(barrier, inc=1, device_id=to, device_id_type=MESH)

        for j in range(1, nx):
            greet(dp=z * nx + lax.rem(x + j, nx))
        pl.when(z >= 1)(lambda: greet(dp=me - nx))
        pl.when(z + 1 < nz)(lambda: greet(dp=me + nx))
        greet(grp=near_grp)
        greet(grp=far_grp)
        pl.semaphore_wait(barrier, nx + 1 + jnp.where(z >= 1, 1, 0) + jnp.where(z + 1 < nz, 1, 0))

    def remote(src, dst, send, recv, **to):
        return pltpu.make_async_remote_copy(
            src_ref=src, dst_ref=dst, send_sem=send, recv_sem=recv, device_id=to, device_id_type=MESH
        )

    def early_tokens():
        return remote(tokens, far_tok.at[aligned(me, rows), :], early_sems[0].at[0], early_sems[1].at[0], grp=far_grp)

    def early_weights(s):
        return remote(
            (w_gate, w_up)[s].at[:, :width], far.at[0, s], early_sems[0].at[1 + s], early_sems[1].at[1 + s], grp=far_grp
        )

    def early_cot(j, own):
        place = far_cot.at[aligned(me, rows), :] if own else stage.at[:, aligned(j, width)]
        return remote(hidden_part(j, 0), place, early_cot_sems[0].at[j], early_cot_sems[1].at[j], grp=far_grp)

    def early():
        copies = [early_tokens(), early_weights(0), early_weights(1)]
        copies += [early_cot(lax.rem(me + j, n), False) for j in range(1, n)]
        return copies + [early_cot(me, True)]

    def relay(buf, sems):
        up_send, up_recv, down_send, down_recv, side_send, side_recv = sems
        piece = rows // PIECES

        def slot(zz, xx, c):
            return buf.at[aligned((zz * nx + xx) * PIECES + c, piece), :]

        def along(zz, c, pair, to):
            place = slot(zz, x, c)
            return remote(place, place, pair[0].at[zz, c], pair[1].at[zz, c], dp=to * nx + x)

        def up(zz, c, back=False):
            return along(zz, c, (up_send, up_recv), z - 1 if back else z + 1)

        def down(zz, c, back=False):
            return along(zz, c, (down_send, down_recv), z + 1 if back else z - 1)

        def side(zz, j, c):
            place = slot(zz, x, c)
            return remote(
                place, place, side_send.at[zz, j - 1, c], side_recv.at[zz, j - 1, c], dp=z * nx + lax.rem(x + j, nx)
            )

        def side_arrival(zz, j, c):
            other = lax.rem(x + nx - j, nx)
            place = slot(zz, other, c)
            return remote(place, place, side_send.at[zz, j - 1, c], side_recv.at[zz, j - 1, c], dp=z * nx + other)

        def pass_on(zz, c, upward):
            if upward is not False:
                pl.when(z + 1 < nz)(lambda: up(zz, c).start())
            if upward is not True:
                pl.when(z >= 1)(lambda: down(zz, c).start())
            for j in range(1, nx):
                side(zz, j, c).start()

        def begin():
            for c in range(PIECES):
                pass_on(z, c, None)

        def turn(r, then):
            for c in range(PIECES):
                @pl.when(z - 1 - r >= 0)
                def _():
                    with jax.named_scope("wait_up"):
                        up(z - 1 - r, c, True).wait_recv()
                    pass_on(z - 1 - r, c, True)

                @pl.when(z + 1 + r < nz)
                def _():
                    with jax.named_scope("wait_down"):
                        down(z + 1 + r, c, True).wait_recv()
                    pass_on(z + 1 + r, c, False)

            pl.when(z - 1 - r >= 0)(lambda: then(z - 1 - r))
            pl.when(z + 1 + r < nz)(lambda: then(z + 1 + r))

        def row_ready(zz):
            for j in range(1, nx):
                for c in range(PIECES):
                    side_arrival(zz, j, c).wait_recv()

        def settle():
            @pl.loop(0, nz)
            def _(zz):
                for c in range(PIECES):
                    for j in range(1, nx):
                        side(zz, j, c).wait_send()
                    pl.when((z + 1 < nz) & (zz <= z))(lambda: up(zz, c).wait_send())
                    pl.when((z >= 1) & (zz >= z))(lambda: down(zz, c).wait_send())

        return begin, turn, row_ready, settle

    def swap(block_of, buf_of, sems):
        def send(to, h):
            return remote(block_of(to, h), buf_of(h).at[aligned(me, rows), :], sems[0].at[h, to], sems[1].at[h, me], dp=to)

        def arrival(source, h):
            place = buf_of(h).at[aligned(source, rows), :]
            return remote(place, place, sems[0].at[h, source], sems[1].at[h, source], dp=source)

        def send_row(zz, h):
            for xx in range(nx):
                pl.when(zz * nx + xx != me)(lambda: send(zz * nx + xx, h).start())

        def row_ready(zz, h):
            for xx in range(nx):
                pl.when(zz * nx + xx != me)(lambda: arrival(zz * nx + xx, h).wait_recv())

        def settle(h):
            @pl.loop(0, n)
            def _(j):
                pl.when(j != me)(lambda: arrival(j, h).wait_send())

        return send_row, row_ready, settle

    least = jnp.minimum(z, nz - 1 - z)
    longer = jnp.where(z < nz - 1 - z, 1, -1)

    def arriving(r):
        near_turn = r <= 2 * least
        step = jnp.where(near_turn, (r + 1) // 2, r - least)
        sign = jnp.where(near_turn, jnp.where(lax.rem(r, 2) == 1, -1, 1), longer)
        return z + sign * step

    def turn_over(buf, turned, zz):
        turned[:, aligned(zz, span)] = buf[aligned(zz, span), :].T

    def project(buf, gate_weight, up_weight, zz):
        part = aligned(zz, span)
        block = buf[part, :]
        gate_pre[part, :] = jnp.dot(block, gate_weight, preferred_element_type=F32) * scale
        up_pre[part, :] = jnp.dot(block, up_weight, preferred_element_type=F32) * scale

    def activate(cotangent, zz):
        part = aligned(zz, span)
        gate = gate_pre[part, :]
        sigma = jax.nn.sigmoid(gate)
        upstream = cotangent[part, :].astype(F32)
        gate_rows[part, :] = (upstream * up_pre[part, :] * sigma * (1.0 + gate * (1.0 - sigma))).astype(BF16)
        up_rows[part, :] = (upstream * gate * sigma).astype(BF16)

    def update(turned, weight, h, i):
        part = aligned(i, BLOCK)
        block = turned[part, :]
        for s, unit_rows in enumerate((gate_rows, up_rows)):
            gradient = jnp.dot(block, unit_rows[...], preferred_element_type=F32) * scale
            weight[h, s, part, :] = (weight[h, s, part, :].astype(F32) - 0.5 * gradient).astype(BF16)

    def near_copy(h, i):
        place = (h, slice(None), aligned(i, BLOCK))
        return remote(held.at[place], near.at[place], near_sems[0].at[h, i], near_sems[1].at[h, i], grp=near_grp)

    def far_copy(h, i):
        place = (h, slice(None), aligned(i, BLOCK))
        return remote(held.at[place], far.at[place], far_sems[0].at[h, i], far_sems[1].at[h, i], grp=far_grp)

    def send_steps(h, i):
        pl.when(even | (h > 0))(lambda: far_copy(h, i).start())
        near_copy(h, i).start()

    @pl.when(odd)
    def _():
        for copy in early():
            copy.start()
        with jax.named_scope("wait_turn"):
            pl.semaphore_wait(turn_sem, 1)

    begin, turn, tokens_ready, settle_tokens = relay(tok, gather_sems)
    send_cot, cot_ready, settle_cot = swap(hidden_part, lambda h: cot.at[h], cot_sems)
    for copy in mine:
        copy.wait()
    begin()
    send_cot(z, 0)

    @pl.loop(0, nz)
    def _(r):
        pl.when(r < nz - 1)(lambda: turn(r, lambda zz: send_cot(zz, 0)))
        zz = arriving(r)
        with jax.named_scope("wait_side"):
            tokens_ready(zz)
        with jax.named_scope("project"):
            turn_over(tok, tok_t, zz)
            project(tok, held[0, 0], held[0, 1], zz)

    @pl.loop(1, slabs)
    def _(h):
        @pl.loop(0, nz)
        def _(r):
            send_cot(arriving(r), h)

    @pl.loop(0, slabs)
    def _(h):
        @pl.when(h > 0)
        def _():
            @pl.loop(0, nz)
            def _(zz):
                project(tok, held[h, 0], held[h, 1], zz)

        @pl.loop(0, nz)
        def _(r):
            zz = arriving(r)
            with jax.named_scope("wait_cot"):
                cot_ready(zz, h)
            with jax.named_scope("forward"):
                activate(cot.at[h], zz)

        @pl.when((h == slabs - 1) & even)
        def _():
            pl.semaphore_signal(turn_sem, inc=1, device_id={"grp": near_grp}, device_id_type=MESH)

        @pl.loop(0, blocks)
        def _(i):
            with jax.named_scope("step"):
                update(tok_t, held, h, i)
            pl.when(i >= 1)(lambda: send_steps(h, i - 1))

        send_steps(h, blocks - 1)

    @pl.when(even)
    def _():
        with jax.named_scope("wait_sibling"):
            near_copy(0, 0).wait_recv()
        for copy in early():
            copy.wait_recv()
        begin, turn, tokens_ready, settle_far_tokens = relay(far_tok, far_gather_sems)
        send_cot, cot_ready, settle_far_cot = swap(
            lambda to, h: stage.at[:, aligned(to, width)], lambda h: far_cot, far_cot_sems
        )
        begin()

        @pl.loop(0, nz)
        def _(r):
            send_cot(arriving(r), 0)

        @pl.loop(0, nz)
        def _(r):
            pl.when(r < nz - 1)(lambda: turn(r, lambda zz: None))
            zz = arriving(r)
            with jax.named_scope("wait_side"):
                tokens_ready(zz)
            with jax.named_scope("forward_far"):
                turn_over(far_tok, far_tok_t, zz)
                project(far_tok, far[0, 0], far[0, 1], zz)

        @pl.loop(0, nz)
        def _(zz):
            with jax.named_scope("wait_cot"):
                cot_ready(zz, 0)
            activate(far_cot, zz)

        @pl.loop(0, blocks)
        def _(i):
            with jax.named_scope("step_far"):
                update(far_tok_t, far, 0, i)

        settle_far_tokens()
        settle_far_cot(0)

    settle_tokens()
    for h in range(slabs):
        settle_cot(h)

    @pl.when(odd)
    def _():
        for copy in early():
            copy.wait_send()

    @pl.loop(0, slabs)
    def _(h):
        @pl.loop(0, blocks)
        def _(i):
            near_copy(h, i).wait_send()
            pl.when(even | (h > 0))(lambda: far_copy(h, i).wait_send())
            with jax.named_scope("wait_near"):
                pl.when(odd | (h > 0) | (i > 0))(lambda: near_copy(h, i).wait_recv())
            with jax.named_scope("wait_far"):
                pl.when(odd | (h > 0))(lambda: far_copy(h, i).wait_recv())
            with jax.named_scope("mix"):
                part = aligned(i, BLOCK)
                for s in range(2):
                    mixed = 0.5 * held[h, s, part, :].astype(F32) + 0.25 * (
                        near[h, s, part, :].astype(F32) + far[h, s, part, :].astype(F32)
                    )
                    far[h, s, part, :] = mixed.astype(BF16)


def place_kernel(mixed, out_gate, out_up, sems):
    slabs, _, _, width = mixed.shape
    copies = [
        pltpu.make_async_copy(mixed.at[h, s], out.at[:, pl.ds(h * width, width)], sems.at[h, s])
        for h in range(slabs)
        for s, out in enumerate((out_gate, out_up))
    ]
    for copy in copies:
        copy.start()
    for copy in copies:
        copy.wait()


def local(tokens, hidden_grad, w_gate, w_up):
    n, groups = lax.axis_size("dp"), lax.axis_size("grp")
    nx = inner_size(n)
    nz = n // nx
    args = [pltpu.with_memory_space_constraint(a[0], pltpu.HBM) for a in (tokens, hidden_grad, w_gate, w_up)]
    rows, depth = args[0].shape
    units = args[2].shape[1]
    total = n * rows
    slabs = slab_count(units)
    width = units // slabs
    blocks = depth // BLOCK
    dma = pltpu.SemaphoreType.DMA
    hops = [dma((nz, PIECES))] * 4 + [dma((nz, max(nx - 1, 1), PIECES))] * 2
    weights = (slabs, 2, depth, width)
    scratch = [
        pltpu.VMEM((total, depth), BF16),
        pltpu.VMEM((depth, total), BF16),
        pltpu.VMEM((slabs, total, width), BF16),
        pltpu.VMEM(weights, BF16),
        pltpu.VMEM(weights, BF16),
        pltpu.VMEM((total, depth), BF16),
        pltpu.VMEM((depth, total), BF16),
        pltpu.VMEM((total, width), BF16),
        pltpu.VMEM((rows, n * width), BF16),
        pltpu.VMEM((total, width), BF16),
        pltpu.VMEM((total, width), BF16),
        pltpu.VMEM((total, width), F32),
        pltpu.VMEM((total, width), F32),
        dma((slabs + 1,)), dma((slabs, 2)), pltpu.SemaphoreType.REGULAR,
        *hops,
        *hops,
        dma((slabs, n)), dma((slabs, n)),
        dma((1, n)), dma((1, n)),
        dma((3,)), dma((3,)),
        dma((n,)), dma((n,)),
        dma((slabs, blocks)), dma((slabs, blocks)),
        dma((slabs, blocks)), dma((slabs, blocks)),
    ]
    mixed = pl.pallas_call(
        functools.partial(kernel, n, groups),
        out_shape=pltpu.VMEM(weights, BF16),
        in_specs=[ANY] * 4,
        out_specs=VMEM,
        scratch_shapes=scratch,
        compiler_params=pltpu.CompilerParams(
            collective_id=0, has_side_effects=True, vmem_limit_bytes=VMEM_LIMIT
        ),
        name="gossip_step",
    )(*args)
    shape = jax.ShapeDtypeStruct((depth, units), BF16)
    outs = pl.pallas_call(
        place_kernel,
        out_shape=[shape, shape],
        in_specs=[VMEM],
        out_specs=[ANY] * 2,
        scratch_shapes=[dma((slabs, 2))],
        compiler_params=pltpu.CompilerParams(vmem_limit_bytes=8 * 1024 * 1024),
        name="place",
    )(pltpu.with_memory_space_constraint(mixed, pltpu.VMEM))
    return tuple(out[None] for out in outs)


def solution(mesh):
    in_specs = (
        P("grp", "dp", None),
        P("grp", "dp", None),
        P("grp", None, "dp"),
        P("grp", None, "dp"),
    )
    out_specs = (P("grp", None, "dp"), P("grp", None, "dp"))
    return jax.shard_map(local, mesh=mesh, in_specs=in_specs, out_specs=out_specs, check_vma=False)
```

```python
import functools

import jax
import jax.numpy as jnp
from jax import lax
from jax.experimental import pallas as pl
from jax.experimental.pallas import tpu as pltpu
from jax.sharding import PartitionSpec as P

LANES = 128
BLOCK = 256
PIECES = 2
VMEM_LIMIT = 54 * 1024 * 1024
VMEM = pl.BlockSpec(memory_space=pltpu.VMEM)
ANY = pl.BlockSpec(memory_space=pl.ANY)
MESH = pl.DeviceIdType.MESH
F32, BF16 = jnp.float32, jnp.bfloat16


def inner_size(n):
    return max(d for d in range(1, n + 1) if n % d == 0 and d * d <= n)


def slab_count(units):
    return next(count for count in (3, 2, 1) if units % (count * LANES) == 0)


def aligned(index, size):
    return pl.ds(pl.multiple_of(index * size, size), size)


def kernel(n, groups, *refs):
    tokens, hidden, w_gate, w_up, far = refs[:5]
    tok, tok_t, cot, held, near, far_tok, far_tok_t, far_cot, stage, gate_rows, up_rows, gate_pre, up_pre = refs[5:18]
    local_sem, turn_sem = refs[18:20]
    gather_sems, far_gather_sems = refs[20:24], refs[24:28]
    cot_sems, far_cot_sems, early_sems, near_sems, far_sems = (refs[k : k + 2] for k in range(28, 38, 2))
    nx = inner_size(n)
    nz = n // nx
    rows, depth = tokens.shape
    units = w_gate.shape[1]
    slabs, _, _, width = held.shape
    scale = depth ** (-0.5)
    blocks = depth // BLOCK
    span = nx * rows
    grp, me = lax.axis_index("grp"), lax.axis_index("dp")
    z, x = me // nx, lax.rem(me, nx)
    odd = lax.rem(grp, 2) == 1
    even = jnp.logical_not(odd)
    near_grp = jnp.where(odd, grp - 1, grp + 1)
    far_grp = jnp.where(odd, lax.rem(grp + 1, groups), lax.rem(grp + groups - 1, groups))

    def hidden_part(to, h):
        return hidden.at[:, pl.ds(pl.multiple_of(to * units + h * width, LANES), width)]

    mine = [pltpu.make_async_copy(tokens, tok.at[aligned(me, rows), :], local_sem.at[0])]
    for h in range(slabs):
        mine.append(pltpu.make_async_copy(hidden_part(me, h), cot.at[h, aligned(me, rows), :], local_sem.at[1]))
        for s, w in enumerate((w_gate, w_up)):
            mine.append(pltpu.make_async_copy(w.at[:, pl.ds(h * width, width)], held.at[h, s], local_sem.at[2]))
    for copy in mine:
        copy.start()

    def wait_mine(k):
        place = (tok.at[aligned(me, rows), :], cot.at[:, aligned(me, rows), :], held)[k]
        pltpu.make_async_copy(place, place, local_sem.at[k]).wait()

    with jax.named_scope("barrier"):
        barrier = pltpu.get_barrier_semaphore()

        def greet(**to):
            pl.semaphore_signal(barrier, inc=1, device_id=to, device_id_type=MESH)

        for j in range(1, nx):
            greet(dp=z * nx + lax.rem(x + j, nx))
        pl.when(z >= 1)(lambda: greet(dp=me - nx))
        pl.when(z + 1 < nz)(lambda: greet(dp=me + nx))
        greet(grp=near_grp)
        greet(grp=far_grp)
        pl.semaphore_wait(barrier, nx + 1 + jnp.where(z >= 1, 1, 0) + jnp.where(z + 1 < nz, 1, 0))

    def remote(src, dst, send, recv, **to):
        return pltpu.make_async_remote_copy(
            src_ref=src, dst_ref=dst, send_sem=send, recv_sem=recv, device_id=to, device_id_type=MESH
        )

    def early(k, src, dst):
        return remote(src, dst, early_sems[0].at[k], early_sems[1].at[k], grp=far_grp)

    def start_early():
        early(0, tokens, far_tok.at[aligned(me, rows), :]).start()
        for s, w in enumerate((w_gate, w_up)):
            early(1, w.at[:, :width], far.at[0, s]).start()
        for j in range(1, n):
            to = lax.rem(me + j, n)
            early(2, hidden_part(to, 0), stage.at[:, aligned(to, width)]).start()
        early(2, hidden_part(me, 0), far_cot.at[0, aligned(me, rows), :]).start()

    def early_whole():
        return [early(k, ref, ref) for k, ref in enumerate((far_tok.at[aligned(me, rows), :], far.at[0], stage))]

    def relay(buf, sems):
        along_send, along_recv, side_send, side_recv = sems
        piece = rows // PIECES

        def slot(zz, xx, c):
            return buf.at[aligned((zz * nx + xx) * PIECES + c, piece), :]

        def along(zz, c, to):
            place = slot(zz, x, c)
            return remote(place, place, along_send, along_recv.at[zz, c], dp=to * nx + x)

        def up(zz, c, back=False):
            return along(zz, c, z - 1 if back else z + 1)

        def down(zz, c, back=False):
            return along(zz, c, z + 1 if back else z - 1)

        def side(zz, j, c):
            place = slot(zz, x, c)
            return remote(place, place, side_send, side_recv.at[zz, j - 1], dp=z * nx + lax.rem(x + j, nx))

        def pass_on(zz, c, upward):
            if upward is not False:
                pl.when(z + 1 < nz)(lambda: up(zz, c).start())
            if upward is not True:
                pl.when(z >= 1)(lambda: down(zz, c).start())
            for j in range(1, nx):
                side(zz, j, c).start()

        def begin():
            for c in range(PIECES):
                pass_on(z, c, None)

        def turn(r, then):
            for c in range(PIECES):
                @pl.when(z - 1 - r >= 0)
                def _():
                    with jax.named_scope("wait_up"):
                        up(z - 1 - r, c, True).wait_recv()
                    pass_on(z - 1 - r, c, True)

                @pl.when(z + 1 + r < nz)
                def _():
                    with jax.named_scope("wait_down"):
                        down(z + 1 + r, c, True).wait_recv()
                    pass_on(z + 1 + r, c, False)

            pl.when(z - 1 - r >= 0)(lambda: then(z - 1 - r))
            pl.when(z + 1 + r < nz)(lambda: then(z + 1 + r))

        def row_ready(zz):
            for j in range(1, nx):
                other = lax.rem(x + nx - j, nx)
                place = buf.at[aligned(zz * nx + other, rows), :]
                remote(place, place, side_send, side_recv.at[zz, j - 1], dp=z * nx + other).wait_recv()

        def settle():
            def sent(count, sem):
                place = buf.at[: count * rows, :]
                remote(place, place, sem, side_recv.at[0, 0], dp=lax.rem(me + 1, n)).wait_send()

            if nx > 1:
                sent(nz * (nx - 1), side_send)
            for at in range(nz):
                count = (at + 1 if at + 1 < nz else 0) + (nz - at if at >= 1 else 0)
                if count > 0:
                    pl.when(z == at)(lambda count=count: sent(count, along_send))

        return begin, turn, row_ready, settle

    def swap(block_of, buf, sems):
        def send_row(zz, h):
            for xx in range(nx):
                to = zz * nx + xx

                @pl.when(to != me)
                def _():
                    remote(
                        block_of(to, h), buf.at[h, aligned(me, rows), :], sems[0].at[0], sems[1].at[h], dp=to
                    ).start()

        def ready(h):
            place = buf.at[h, : (n - 1) * rows, :]
            remote(place, place, sems[0].at[0], sems[1].at[h], dp=lax.rem(me + 1, n)).wait_recv()

        def settle():
            place = buf.at[:, : (n - 1) * rows, :]
            remote(place, place, sems[0].at[0], sems[1].at[0], dp=lax.rem(me + 1, n)).wait_send()

        return send_row, ready, settle

    least = jnp.minimum(z, nz - 1 - z)
    longer = jnp.where(z < nz - 1 - z, 1, -1)

    def arriving(r):
        near_turn = r <= 2 * least
        step = jnp.where(near_turn, (r + 1) // 2, r - least)
        sign = jnp.where(near_turn, jnp.where(lax.rem(r, 2) == 1, -1, 1), longer)
        return z + sign * step

    def turn_over(buf, turned, zz):
        turned[:, aligned(zz, span)] = buf[aligned(zz, span), :].T

    def project(buf, gate_weight, up_weight, zz):
        part = aligned(zz, span)
        block = buf[part, :]
        gate_pre[part, :] = jnp.dot(block, gate_weight, preferred_element_type=F32) * scale
        up_pre[part, :] = jnp.dot(block, up_weight, preferred_element_type=F32) * scale

    def activate(cotangent, zz):
        part = aligned(zz, span)
        gate = gate_pre[part, :]
        sigma = jax.nn.sigmoid(gate)
        upstream = cotangent[part, :].astype(F32)
        gate_rows[part, :] = (upstream * up_pre[part, :] * sigma * (1.0 + gate * (1.0 - sigma))).astype(BF16)
        up_rows[part, :] = (upstream * gate * sigma).astype(BF16)

    def update(turned, weight, h, i):
        part = aligned(i, BLOCK)
        block = turned[part, :]
        for s, unit_rows in enumerate((gate_rows, up_rows)):
            gradient = jnp.dot(block, unit_rows[...], preferred_element_type=F32) * scale
            weight[h, s, part, :] = (weight[h, s, part, :].astype(F32) - 0.5 * gradient).astype(BF16)

    def near_copy(h, i):
        place = (h, slice(None), aligned(i, BLOCK))
        return remote(held.at[place], near.at[place], near_sems[0].at[0], near_sems[1].at[h], grp=near_grp)

    def near_slab(h):
        return remote(held.at[h], near.at[h], near_sems[0].at[0], near_sems[1].at[h], grp=near_grp)

    def far_copy(h, i):
        place = (h, slice(None), aligned(i, BLOCK))
        k = jnp.where(h == slabs - 1, h + i, h)
        return remote(held.at[place], far.at[place], far_sems[0].at[0], far_sems[1].at[k], grp=far_grp)

    def far_slab(h):
        return remote(held.at[h], far.at[h], far_sems[0].at[0], far_sems[1].at[h], grp=far_grp)

    def far_sent(first):
        place = pl.ds(first, slabs - first)
        remote(held.at[place], far.at[place], far_sems[0].at[0], far_sems[1].at[0], grp=far_grp).wait_send()

    def send_steps(h, i):
        pl.when(even | (h > 0))(lambda: far_copy(h, i).start())
        near_copy(h, i).start()

    @pl.when(odd)
    def _():
        start_early()
        with jax.named_scope("wait_turn"):
            pl.semaphore_wait(turn_sem, 1)

    begin, turn, tokens_ready, settle_tokens = relay(tok, gather_sems)
    send_cot, cot_ready, settle_cot = swap(hidden_part, cot, cot_sems)
    wait_mine(0)
    begin()
    send_cot(z, 0)
    wait_mine(1)
    wait_mine(2)

    @pl.loop(0, nz)
    def _(r):
        pl.when(r < nz - 1)(lambda: turn(r, lambda zz: send_cot(zz, 0)))
        zz = arriving(r)
        with jax.named_scope("wait_side"):
            tokens_ready(zz)
        with jax.named_scope("project"):
            turn_over(tok, tok_t, zz)
            project(tok, held[0, 0], held[0, 1], zz)

    @pl.loop(1, slabs)
    def _(h):
        @pl.loop(0, nz)
        def _(r):
            send_cot(arriving(r), h)

    @pl.loop(0, slabs)
    def _(h):
        @pl.when(h > 0)
        def _():
            @pl.loop(0, nz)
            def _(zz):
                project(tok, held[h, 0], held[h, 1], zz)

        with jax.named_scope("wait_cot"):
            cot_ready(h)

        @pl.loop(0, nz)
        def _(zz):
            with jax.named_scope("forward"):
                activate(cot.at[h], zz)

        @pl.when((h == slabs - 1) & even)
        def _():
            pl.semaphore_signal(turn_sem, inc=1, device_id={"grp": near_grp}, device_id_type=MESH)

        @pl.loop(0, blocks)
        def _(i):
            with jax.named_scope("step"):
                update(tok_t, held, h, i)
            pl.when(i >= 1)(lambda: send_steps(h, i - 1))

        send_steps(h, blocks - 1)

    @pl.when(even)
    def _():
        with jax.named_scope("wait_sibling"):
            near_slab(0).wait_recv()
        for copy in early_whole():
            copy.wait_recv()
        begin, turn, tokens_ready, settle_far_tokens = relay(far_tok, far_gather_sems)
        send_cot, cot_ready, settle_far_cot = swap(
            lambda to, h: stage.at[:, aligned(to, width)], far_cot, far_cot_sems
        )
        begin()

        @pl.loop(0, nz)
        def _(r):
            send_cot(arriving(r), 0)

        @pl.loop(0, nz)
        def _(r):
            pl.when(r < nz - 1)(lambda: turn(r, lambda zz: None))
            zz = arriving(r)
            with jax.named_scope("wait_side"):
                tokens_ready(zz)
            with jax.named_scope("forward_far"):
                turn_over(far_tok, far_tok_t, zz)
                project(far_tok, far[0, 0], far[0, 1], zz)

        with jax.named_scope("wait_cot"):
            cot_ready(0)

        @pl.loop(0, nz)
        def _(zz):
            activate(far_cot.at[0], zz)

        @pl.loop(0, blocks)
        def _(i):
            with jax.named_scope("step_far"):
                update(far_tok_t, far, 0, i)

        settle_far_tokens()
        settle_far_cot()

    settle_tokens()
    settle_cot()

    @pl.when(odd)
    def _():
        for copy in early_whole():
            copy.wait_send()

    @pl.loop(0, slabs)
    def _(h):
        with jax.named_scope("wait_near"):
            pl.when(odd | (h > 0))(lambda: near_slab(h).wait_recv())
        pl.when((h < slabs - 1) & (odd | (h > 0)))(lambda: far_slab(h).wait_recv())

        @pl.when(h == slabs - 1)
        def _():
            remote(held, near, near_sems[0].at[0], near_sems[1].at[0], grp=near_grp).wait_send()
            pl.when(even)(lambda: far_sent(0))

        @pl.loop(0, blocks)
        def _(i):
            with jax.named_scope("wait_far"):
                pl.when(h == slabs - 1)(lambda: far_copy(h, i).wait_recv())
            with jax.named_scope("mix"):
                part = aligned(i, BLOCK)
                for s in range(2):
                    mixed = 0.5 * held[h, s, part, :].astype(F32) + 0.25 * (
                        near[h, s, part, :].astype(F32) + far[h, s, part, :].astype(F32)
                    )
                    far[h, s, part, :] = mixed.astype(BF16)

    pl.when(odd)(lambda: far_sent(1))


def place_kernel(mixed, out_gate, out_up, sems):
    slabs, _, _, width = mixed.shape
    copies = [
        pltpu.make_async_copy(mixed.at[h, s], out.at[:, pl.ds(h * width, width)], sems.at[h, s])
        for h in range(slabs)
        for s, out in enumerate((out_gate, out_up))
    ]
    for copy in copies:
        copy.start()
    for copy in copies:
        copy.wait()


def local(tokens, hidden_grad, w_gate, w_up):
    n, groups = lax.axis_size("dp"), lax.axis_size("grp")
    nx = inner_size(n)
    nz = n // nx
    args = [pltpu.with_memory_space_constraint(a[0], pltpu.HBM) for a in (tokens, hidden_grad, w_gate, w_up)]
    rows, depth = args[0].shape
    units = args[2].shape[1]
    total = n * rows
    slabs = slab_count(units)
    width = units // slabs
    blocks = depth // BLOCK
    dma = pltpu.SemaphoreType.DMA
    hops = [dma, dma((nz, PIECES)), dma, dma((nz, max(nx - 1, 1)))]
    weights = (slabs, 2, depth, width)
    scratch = [
        pltpu.VMEM((total, depth), BF16),
        pltpu.VMEM((depth, total), BF16),
        pltpu.VMEM((slabs, total, width), BF16),
        pltpu.VMEM(weights, BF16),
        pltpu.VMEM(weights, BF16),
        pltpu.VMEM((total, depth), BF16),
        pltpu.VMEM((depth, total), BF16),
        pltpu.VMEM((1, total, width), BF16),
        pltpu.VMEM((rows, n * width), BF16),
        pltpu.VMEM((total, width), BF16),
        pltpu.VMEM((total, width), BF16),
        pltpu.VMEM((total, width), F32),
        pltpu.VMEM((total, width), F32),
        dma((3,)), pltpu.SemaphoreType.REGULAR,
        *hops,
        *hops,
        dma((1,)), dma((slabs,)),
        dma((1,)), dma((1,)),
        dma((3,)), dma((3,)),
        dma((1,)), dma((slabs,)),
        dma((1,)), dma((slabs - 1 + blocks,)),
    ]
    mixed = pl.pallas_call(
        functools.partial(kernel, n, groups),
        out_shape=pltpu.VMEM(weights, BF16),
        in_specs=[ANY] * 4,
        out_specs=VMEM,
        scratch_shapes=scratch,
        compiler_params=pltpu.CompilerParams(
            collective_id=0, has_side_effects=True, vmem_limit_bytes=VMEM_LIMIT
        ),
        name="gossip_step",
    )(*args)
    shape = jax.ShapeDtypeStruct((depth, units), BF16)
    outs = pl.pallas_call(
        place_kernel,
        out_shape=[shape, shape],
        in_specs=[VMEM],
        out_specs=[ANY] * 2,
        scratch_shapes=[dma((slabs, 2))],
        compiler_params=pltpu.CompilerParams(vmem_limit_bytes=8 * 1024 * 1024),
        name="place",
    )(pltpu.with_memory_space_constraint(mixed, pltpu.VMEM))
    return tuple(out[None] for out in outs)


def solution(mesh):
    in_specs = (
        P("grp", "dp", None),
        P("grp", "dp", None),
        P("grp", None, "dp"),
        P("grp", None, "dp"),
    )
    out_specs = (P("grp", None, "dp"), P("grp", None, "dp"))
    return jax.shard_map(local, mesh=mesh, in_specs=in_specs, out_specs=out_specs, check_vma=False)
```

```python
import functools

import jax
import jax.numpy as jnp
from jax import lax
from jax.experimental import pallas as pl
from jax.experimental.pallas import tpu as pltpu
from jax.sharding import PartitionSpec as P

LANES = 128
BLOCK = 256
PIECES = 2
VMEM_LIMIT = 54 * 1024 * 1024
VMEM = pl.BlockSpec(memory_space=pltpu.VMEM)
ANY = pl.BlockSpec(memory_space=pl.ANY)
MESH = pl.DeviceIdType.MESH
F32, BF16 = jnp.float32, jnp.bfloat16


def inner_size(n):
    return max(d for d in range(1, n + 1) if n % d == 0 and d * d <= n)


def slab_count(units):
    return next(count for count in (3, 2, 1) if units % (count * LANES) == 0)


def aligned(index, size):
    return pl.ds(pl.multiple_of(index * size, size), size)


def kernel(n, groups, *refs):
    tokens, hidden, w_gate, w_up, far = refs[:5]
    tok, tok_t, cot, held, near, far_tok, far_tok_t, far_cot, stage, gate_rows, up_rows, gate_pre, up_pre = refs[5:18]
    local_sem, turn_sem = refs[18:20]
    gather_sems, far_gather_sems = refs[20:24], refs[24:28]
    cot_sems, far_cot_sems, early_sems, near_sems, far_sems = (refs[k : k + 2] for k in range(28, 38, 2))
    nx = inner_size(n)
    nz = n // nx
    rows, depth = tokens.shape
    units = w_gate.shape[1]
    slabs, _, _, width = held.shape
    scale = depth ** (-0.5)
    blocks = depth // BLOCK
    span = nx * rows
    grp, me = lax.axis_index("grp"), lax.axis_index("dp")
    z, x = me // nx, lax.rem(me, nx)
    odd = lax.rem(grp, 2) == 1
    even = jnp.logical_not(odd)
    near_grp = jnp.where(odd, grp - 1, grp + 1)
    far_grp = jnp.where(odd, lax.rem(grp + 1, groups), lax.rem(grp + groups - 1, groups))

    def hidden_part(to, h):
        return hidden.at[:, pl.ds(pl.multiple_of(to * units + h * width, LANES), width)]

    mine = [pltpu.make_async_copy(tokens, tok.at[aligned(me, rows), :], local_sem.at[0])]
    for h in range(slabs):
        mine.append(pltpu.make_async_copy(hidden_part(me, h), cot.at[h, aligned(me, rows), :], local_sem.at[1]))
        for s, w in enumerate((w_gate, w_up)):
            mine.append(pltpu.make_async_copy(w.at[:, pl.ds(h * width, width)], held.at[h, s], local_sem.at[2]))
    for copy in mine:
        copy.start()

    def wait_mine(k):
        place = (tok.at[aligned(me, rows), :], cot.at[:, aligned(me, rows), :], held)[k]
        pltpu.make_async_copy(place, place, local_sem.at[k]).wait()

    with jax.named_scope("barrier"):
        barrier = pltpu.get_barrier_semaphore()

        def greet(**to):
            pl.semaphore_signal(barrier, inc=1, device_id=to, device_id_type=MESH)

        greet(grp=far_grp)

        @pl.when(odd)
        def _():
            greet(grp=near_grp)
            pl.semaphore_wait(barrier, 1)

        @pl.when(even)
        def _():
            for j in range(1, nx):
                greet(dp=z * nx + lax.rem(x + j, nx))
            pl.when(z >= 1)(lambda: greet(dp=me - nx))
            pl.when(z + 1 < nz)(lambda: greet(dp=me + nx))
            pl.semaphore_wait(barrier, nx + 1 + jnp.where(z >= 1, 1, 0) + jnp.where(z + 1 < nz, 1, 0))

    def remote(src, dst, send, recv, **to):
        return pltpu.make_async_remote_copy(
            src_ref=src, dst_ref=dst, send_sem=send, recv_sem=recv, device_id=to, device_id_type=MESH
        )

    def early(k, src, dst):
        return remote(src, dst, early_sems[0].at[k], early_sems[1].at[k], grp=far_grp)

    def start_early():
        early(0, tokens, far_tok.at[aligned(me, rows), :]).start()
        for s, w in enumerate((w_gate, w_up)):
            early(1, w.at[:, :width], far.at[0, s]).start()
        for j in range(1, n):
            to = lax.rem(me + j, n)
            early(2, hidden_part(to, 0), stage.at[:, aligned(to, width)]).start()
        early(2, hidden_part(me, 0), far_cot.at[0, aligned(me, rows), :]).start()

    def early_whole():
        return [early(k, ref, ref) for k, ref in enumerate((far_tok.at[aligned(me, rows), :], far.at[0], stage))]

    def relay(buf, sems):
        along_send, along_recv, side_send, side_recv = sems
        piece = rows // PIECES

        def slot(zz, xx, c):
            return buf.at[aligned((zz * nx + xx) * PIECES + c, piece), :]

        def along(zz, c, to):
            place = slot(zz, x, c)
            return remote(place, place, along_send, along_recv.at[zz, c], dp=to * nx + x)

        def up(zz, c, back=False):
            return along(zz, c, z - 1 if back else z + 1)

        def down(zz, c, back=False):
            return along(zz, c, z + 1 if back else z - 1)

        def side(zz, j, c):
            place = slot(zz, x, c)
            return remote(place, place, side_send, side_recv.at[zz, j - 1], dp=z * nx + lax.rem(x + j, nx))

        def pass_on(zz, c, upward):
            if upward is not False:
                pl.when(z + 1 < nz)(lambda: up(zz, c).start())
            if upward is not True:
                pl.when(z >= 1)(lambda: down(zz, c).start())
            for j in range(1, nx):
                side(zz, j, c).start()

        def begin():
            for c in range(PIECES):
                pass_on(z, c, None)

        def turn(r, then):
            for c in range(PIECES):
                @pl.when(z - 1 - r >= 0)
                def _():
                    with jax.named_scope("wait_up"):
                        up(z - 1 - r, c, True).wait_recv()
                    pass_on(z - 1 - r, c, True)

                @pl.when(z + 1 + r < nz)
                def _():
                    with jax.named_scope("wait_down"):
                        down(z + 1 + r, c, True).wait_recv()
                    pass_on(z + 1 + r, c, False)

            pl.when(z - 1 - r >= 0)(lambda: then(z - 1 - r))
            pl.when(z + 1 + r < nz)(lambda: then(z + 1 + r))

        def row_ready(zz):
            for j in range(1, nx):
                other = lax.rem(x + nx - j, nx)
                place = buf.at[aligned(zz * nx + other, rows), :]
                remote(place, place, side_send, side_recv.at[zz, j - 1], dp=z * nx + other).wait_recv()

        def settle():
            def sent(count, sem):
                place = buf.at[: count * rows, :]
                remote(place, place, sem, side_recv.at[0, 0], dp=lax.rem(me + 1, n)).wait_send()

            if nx > 1:
                sent(nz * (nx - 1), side_send)
            for at in range(nz):
                count = (at + 1 if at + 1 < nz else 0) + (nz - at if at >= 1 else 0)
                if count > 0:
                    pl.when(z == at)(lambda count=count: sent(count, along_send))

        return begin, turn, row_ready, settle

    def swap(block_of, buf, sems):
        def send_row(zz, h):
            for xx in range(nx):
                to = zz * nx + xx

                @pl.when(to != me)
                def _():
                    remote(
                        block_of(to, h), buf.at[h, aligned(me, rows), :], sems[0].at[0], sems[1].at[h], dp=to
                    ).start()

        def ready(h):
            place = buf.at[h, : (n - 1) * rows, :]
            remote(place, place, sems[0].at[0], sems[1].at[h], dp=lax.rem(me + 1, n)).wait_recv()

        def settle():
            place = buf.at[:, : (n - 1) * rows, :]
            remote(place, place, sems[0].at[0], sems[1].at[0], dp=lax.rem(me + 1, n)).wait_send()

        return send_row, ready, settle

    least = jnp.minimum(z, nz - 1 - z)
    longer = jnp.where(z < nz - 1 - z, 1, -1)

    def arriving(r):
        near_turn = r <= 2 * least
        step = jnp.where(near_turn, (r + 1) // 2, r - least)
        sign = jnp.where(near_turn, jnp.where(lax.rem(r, 2) == 1, -1, 1), longer)
        return z + sign * step

    def turn_over(buf, turned, zz):
        turned[:, aligned(zz, span)] = buf[aligned(zz, span), :].T

    def project(buf, gate_weight, up_weight, zz):
        part = aligned(zz, span)
        block = buf[part, :]
        gate_pre[part, :] = jnp.dot(block, gate_weight, preferred_element_type=F32) * scale
        up_pre[part, :] = jnp.dot(block, up_weight, preferred_element_type=F32) * scale

    def activate(cotangent, zz):
        part = aligned(zz, span)
        gate = gate_pre[part, :]
        sigma = jax.nn.sigmoid(gate)
        upstream = cotangent[part, :].astype(F32)
        gate_rows[part, :] = (upstream * up_pre[part, :] * sigma * (1.0 + gate * (1.0 - sigma))).astype(BF16)
        up_rows[part, :] = (upstream * gate * sigma).astype(BF16)

    def update(turned, weight, h, i):
        part = aligned(i, BLOCK)
        block = turned[part, :]
        for s, unit_rows in enumerate((gate_rows, up_rows)):
            gradient = jnp.dot(block, unit_rows[...], preferred_element_type=F32) * scale
            weight[h, s, part, :] = (weight[h, s, part, :].astype(F32) - 0.5 * gradient).astype(BF16)

    def near_copy(h, i):
        place = (h, slice(None), aligned(i, BLOCK))
        return remote(held.at[place], near.at[place], near_sems[0].at[0], near_sems[1].at[h], grp=near_grp)

    def near_slab(h):
        return remote(held.at[h], near.at[h], near_sems[0].at[0], near_sems[1].at[h], grp=near_grp)

    def far_copy(h, i):
        place = (h, slice(None), aligned(i, BLOCK))
        k = jnp.where(h == slabs - 1, h + i, h)
        return remote(held.at[place], far.at[place], far_sems[0].at[0], far_sems[1].at[k], grp=far_grp)

    def far_slab(h):
        return remote(held.at[h], far.at[h], far_sems[0].at[0], far_sems[1].at[h], grp=far_grp)

    def far_sent(first):
        place = pl.ds(first, slabs - first)
        remote(held.at[place], far.at[place], far_sems[0].at[0], far_sems[1].at[0], grp=far_grp).wait_send()

    def send_steps(h, i):
        pl.when(even | (h > 0))(lambda: far_copy(h, i).start())
        near_copy(h, i).start()

    @pl.when(odd)
    def _():
        start_early()
        with jax.named_scope("wait_turn"):
            pl.semaphore_wait(turn_sem, 1)

    begin, turn, tokens_ready, settle_tokens = relay(tok, gather_sems)
    send_cot, cot_ready, settle_cot = swap(hidden_part, cot, cot_sems)
    wait_mine(0)
    begin()
    send_cot(z, 0)
    wait_mine(1)
    wait_mine(2)

    @pl.loop(0, nz)
    def _(r):
        pl.when(r < nz - 1)(lambda: turn(r, lambda zz: send_cot(zz, 0)))
        zz = arriving(r)
        with jax.named_scope("wait_side"):
            tokens_ready(zz)
        with jax.named_scope("project"):
            turn_over(tok, tok_t, zz)
            project(tok, held[0, 0], held[0, 1], zz)

    @pl.loop(1, slabs)
    def _(h):
        @pl.loop(0, nz)
        def _(r):
            send_cot(arriving(r), h)

    @pl.loop(0, slabs)
    def _(h):
        @pl.when(h > 0)
        def _():
            @pl.loop(0, nz)
            def _(zz):
                project(tok, held[h, 0], held[h, 1], zz)

        with jax.named_scope("wait_cot"):
            cot_ready(h)

        @pl.loop(0, nz)
        def _(zz):
            with jax.named_scope("forward"):
                activate(cot.at[h], zz)

        @pl.when((h == slabs - 1) & even)
        def _():
            pl.semaphore_signal(turn_sem, inc=1, device_id={"grp": near_grp}, device_id_type=MESH)

        @pl.loop(0, blocks)
        def _(i):
            with jax.named_scope("step"):
                update(tok_t, held, h, i)
            pl.when(i >= 1)(lambda: send_steps(h, i - 1))

        send_steps(h, blocks - 1)

    @pl.when(even)
    def _():
        with jax.named_scope("wait_sibling"):
            near_slab(0).wait_recv()
        for copy in early_whole():
            copy.wait_recv()
        begin, turn, tokens_ready, settle_far_tokens = relay(far_tok, far_gather_sems)
        send_cot, cot_ready, settle_far_cot = swap(
            lambda to, h: stage.at[:, aligned(to, width)], far_cot, far_cot_sems
        )
        begin()

        @pl.loop(0, nz)
        def _(r):
            send_cot(arriving(r), 0)

        @pl.loop(0, nz)
        def _(r):
            pl.when(r < nz - 1)(lambda: turn(r, lambda zz: None))
            zz = arriving(r)
            with jax.named_scope("wait_side"):
                tokens_ready(zz)
            with jax.named_scope("forward_far"):
                turn_over(far_tok, far_tok_t, zz)
                project(far_tok, far[0, 0], far[0, 1], zz)

        with jax.named_scope("wait_cot"):
            cot_ready(0)

        @pl.loop(0, nz)
        def _(zz):
            activate(far_cot.at[0], zz)

        @pl.loop(0, blocks)
        def _(i):
            with jax.named_scope("step_far"):
                update(far_tok_t, far, 0, i)

        settle_far_tokens()
        settle_far_cot()

    settle_tokens()
    settle_cot()

    @pl.when(odd)
    def _():
        for copy in early_whole():
            copy.wait_send()

    @pl.loop(0, slabs)
    def _(h):
        with jax.named_scope("wait_near"):
            pl.when(odd | (h > 0))(lambda: near_slab(h).wait_recv())
        pl.when((h < slabs - 1) & (odd | (h > 0)))(lambda: far_slab(h).wait_recv())

        @pl.when(h == slabs - 1)
        def _():
            remote(held, near, near_sems[0].at[0], near_sems[1].at[0], grp=near_grp).wait_send()
            pl.when(even)(lambda: far_sent(0))

        @pl.loop(0, blocks)
        def _(i):
            with jax.named_scope("wait_far"):
                pl.when(h == slabs - 1)(lambda: far_copy(h, i).wait_recv())
            with jax.named_scope("mix"):
                part = aligned(i, BLOCK)
                for s in range(2):
                    mixed = 0.5 * held[h, s, part, :].astype(F32) + 0.25 * (
                        near[h, s, part, :].astype(F32) + far[h, s, part, :].astype(F32)
                    )
                    far[h, s, part, :] = mixed.astype(BF16)

    pl.when(odd)(lambda: far_sent(1))


def place_kernel(mixed, out_gate, out_up, sems):
    slabs, _, _, width = mixed.shape
    copies = [
        pltpu.make_async_copy(mixed.at[h, s], out.at[:, pl.ds(h * width, width)], sems.at[h, s])
        for h in range(slabs)
        for s, out in enumerate((out_gate, out_up))
    ]
    for copy in copies:
        copy.start()
    for copy in copies:
        copy.wait()


def local(tokens, hidden_grad, w_gate, w_up):
    n, groups = lax.axis_size("dp"), lax.axis_size("grp")
    nx = inner_size(n)
    nz = n // nx
    args = [pltpu.with_memory_space_constraint(a[0], pltpu.HBM) for a in (tokens, hidden_grad, w_gate, w_up)]
    rows, depth = args[0].shape
    units = args[2].shape[1]
    total = n * rows
    slabs = slab_count(units)
    width = units // slabs
    blocks = depth // BLOCK
    dma = pltpu.SemaphoreType.DMA
    hops = [dma, dma((nz, PIECES)), dma, dma((nz, max(nx - 1, 1)))]
    weights = (slabs, 2, depth, width)
    scratch = [
        pltpu.VMEM((total, depth), BF16),
        pltpu.VMEM((depth, total), BF16),
        pltpu.VMEM((slabs, total, width), BF16),
        pltpu.VMEM(weights, BF16),
        pltpu.VMEM(weights, BF16),
        pltpu.VMEM((total, depth), BF16),
        pltpu.VMEM((depth, total), BF16),
        pltpu.VMEM((1, total, width), BF16),
        pltpu.VMEM((rows, n * width), BF16),
        pltpu.VMEM((total, width), BF16),
        pltpu.VMEM((total, width), BF16),
        pltpu.VMEM((total, width), F32),
        pltpu.VMEM((total, width), F32),
        dma((3,)), pltpu.SemaphoreType.REGULAR,
        *hops,
        *hops,
        dma((1,)), dma((slabs,)),
        dma((1,)), dma((1,)),
        dma((3,)), dma((3,)),
        dma((1,)), dma((slabs,)),
        dma((1,)), dma((slabs - 1 + blocks,)),
    ]
    mixed = pl.pallas_call(
        functools.partial(kernel, n, groups),
        out_shape=pltpu.VMEM(weights, BF16),
        in_specs=[ANY] * 4,
        out_specs=VMEM,
        scratch_shapes=scratch,
        compiler_params=pltpu.CompilerParams(
            collective_id=0, has_side_effects=True, vmem_limit_bytes=VMEM_LIMIT
        ),
        name="gossip_step",
    )(*args)
    shape = jax.ShapeDtypeStruct((depth, units), BF16)
    outs = pl.pallas_call(
        place_kernel,
        out_shape=[shape, shape],
        in_specs=[VMEM],
        out_specs=[ANY] * 2,
        scratch_shapes=[dma((slabs, 2))],
        compiler_params=pltpu.CompilerParams(vmem_limit_bytes=8 * 1024 * 1024),
        name="place",
    )(pltpu.with_memory_space_constraint(mixed, pltpu.VMEM))
    return tuple(out[None] for out in outs)


def solution(mesh):
    in_specs = (
        P("grp", "dp", None),
        P("grp", "dp", None),
        P("grp", None, "dp"),
        P("grp", None, "dp"),
    )
    out_specs = (P("grp", None, "dp"), P("grp", None, "dp"))
    return jax.shard_map(local, mesh=mesh, in_specs=in_specs, out_specs=out_specs, check_vma=False)
```

```python
import functools

import jax
import jax.numpy as jnp
from jax import lax
from jax.experimental import pallas as pl
from jax.experimental.pallas import tpu as pltpu
from jax.sharding import PartitionSpec as P

LANES = 128
BLOCK = 256
PIECES = 2
WRITES = 4
VMEM_LIMIT = 54 * 1024 * 1024
VMEM = pl.BlockSpec(memory_space=pltpu.VMEM)
ANY = pl.BlockSpec(memory_space=pl.ANY)
MESH = pl.DeviceIdType.MESH
F32, BF16 = jnp.float32, jnp.bfloat16


def inner_size(n):
    return max(d for d in range(1, n + 1) if n % d == 0 and d * d <= n)


def slab_count(units):
    return next(count for count in (3, 2, 1) if units % (count * LANES) == 0)


def aligned(index, size):
    return pl.ds(pl.multiple_of(index * size, size), size)


def kernel(n, groups, *refs):
    tokens, hidden, w_gate, w_up, far = refs[:5]
    tok, tok_t, cot, held, near, far_tok, far_tok_t, far_cot, stage, gate_rows, up_rows, gate_pre, up_pre = refs[5:18]
    local_sem, turn_sem = refs[18:20]
    gather_sems = refs[20:24]
    cot_sems, early_sems, near_sems, far_sems = (refs[k : k + 2] for k in range(24, 32, 2))
    nx = inner_size(n)
    nz = n // nx
    rows, depth = tokens.shape
    units = w_gate.shape[1]
    slabs, _, _, width = held.shape
    scale = depth ** (-0.5)
    blocks = depth // BLOCK
    span = nx * rows
    grp, me = lax.axis_index("grp"), lax.axis_index("dp")
    z, x = me // nx, lax.rem(me, nx)
    odd = lax.rem(grp, 2) == 1
    even = jnp.logical_not(odd)
    near_grp = jnp.where(odd, grp - 1, grp + 1)
    far_grp = jnp.where(odd, lax.rem(grp + 1, groups), lax.rem(grp + groups - 1, groups))

    def hidden_part(to, h):
        return hidden.at[:, pl.ds(pl.multiple_of(to * units + h * width, LANES), width)]

    def wait_mine(k):
        place = (tok.at[aligned(me, rows), :], cot.at[:, aligned(me, rows), :], held)[k]
        pltpu.make_async_copy(place, place, local_sem.at[k]).wait()

    barrier = pltpu.get_barrier_semaphore()

    def greet(**to):
        pl.semaphore_signal(barrier, inc=1, device_id=to, device_id_type=MESH)

    greet(grp=far_grp)
    pl.when(odd)(lambda: greet(grp=near_grp))

    @pl.when(even)
    def _():
        for j in range(1, nx):
            greet(dp=z * nx + lax.rem(x + j, nx))
        pl.when(z >= 1)(lambda: greet(dp=me - nx))
        pl.when(z + 1 < nz)(lambda: greet(dp=me + nx))

    mine = [pltpu.make_async_copy(tokens, tok.at[aligned(me, rows), :], local_sem.at[0])]
    for h in range(slabs):
        mine.append(pltpu.make_async_copy(hidden_part(me, h), cot.at[h, aligned(me, rows), :], local_sem.at[1]))
        for s, w in enumerate((w_gate, w_up)):
            mine.append(pltpu.make_async_copy(w.at[:, pl.ds(h * width, width)], held.at[h, s], local_sem.at[2]))
    for copy in mine:
        copy.start()

    with jax.named_scope("barrier"):
        expected = nx + 1 + jnp.where(z >= 1, 1, 0) + jnp.where(z + 1 < nz, 1, 0)
        pl.semaphore_wait(barrier, jnp.where(odd, 1, expected))

    def remote(src, dst, send, recv, **to):
        return pltpu.make_async_remote_copy(
            src_ref=src, dst_ref=dst, send_sem=send, recv_sem=recv, device_id=to, device_id_type=MESH
        )

    def early(k, src, dst):
        return remote(src, dst, early_sems[0].at[k], early_sems[1].at[k], grp=far_grp)

    def start_early():
        place = aligned(me, rows)
        early(0, tokens, far_tok.at[place, :]).start()
        for s, w in enumerate((w_gate, w_up)):
            early(1, w.at[:, :width], far.at[0, s]).start()
        for j in range(1, n):
            to = lax.rem(me + j, n)
            early(2, hidden_part(to, 0), stage.at[:, aligned(to, width)]).start()
        early(2, hidden_part(me, 0), far_cot.at[0, aligned(me, rows), :]).start()

    def early_whole():
        return [early(k, ref, ref) for k, ref in enumerate((far_tok.at[aligned(me, rows), :], far.at[0], stage))]

    def relay(buf, sems):
        along_send, along_recv, side_send, side_recv = sems
        piece = rows // PIECES

        def slot(zz, xx, c):
            return buf.at[aligned((zz * nx + xx) * PIECES + c, piece), :]

        def along(zz, c, to):
            place = slot(zz, x, c)
            return remote(place, place, along_send, along_recv.at[zz, c], dp=to * nx + x)

        def up(zz, c, back=False):
            return along(zz, c, z - 1 if back else z + 1)

        def down(zz, c, back=False):
            return along(zz, c, z + 1 if back else z - 1)

        def side(zz, j, c):
            place = slot(zz, x, c)
            return remote(place, place, side_send, side_recv.at[zz, j - 1], dp=z * nx + lax.rem(x + j, nx))

        def pass_on(zz, c, upward):
            if upward is not False:
                pl.when(z + 1 < nz)(lambda: up(zz, c).start())
            if upward is not True:
                pl.when(z >= 1)(lambda: down(zz, c).start())
            for j in range(1, nx):
                side(zz, j, c).start()

        def begin():
            for c in range(PIECES):
                pass_on(z, c, None)

        def turn(r, then):
            for c in range(PIECES):
                @pl.when(z - 1 - r >= 0)
                def _():
                    with jax.named_scope("wait_up"):
                        up(z - 1 - r, c, True).wait_recv()
                    pass_on(z - 1 - r, c, True)

                @pl.when(z + 1 + r < nz)
                def _():
                    with jax.named_scope("wait_down"):
                        down(z + 1 + r, c, True).wait_recv()
                    pass_on(z + 1 + r, c, False)

            pl.when(z - 1 - r >= 0)(lambda: then(z - 1 - r))
            pl.when(z + 1 + r < nz)(lambda: then(z + 1 + r))

        def row_ready(zz):
            for j in range(1, nx):
                other = lax.rem(x + nx - j, nx)
                place = buf.at[aligned(zz * nx + other, rows), :]
                remote(place, place, side_send, side_recv.at[zz, j - 1], dp=z * nx + other).wait_recv()

        def settle():
            def sent(count, sem):
                place = buf.at[: count * rows, :]
                remote(place, place, sem, side_recv.at[0, 0], dp=lax.rem(me + 1, n)).wait_send()

            if nx > 1:
                sent(nz * (nx - 1), side_send)
            for at in range(nz):
                count = (at + 1 if at + 1 < nz else 0) + (nz - at if at >= 1 else 0)
                if count > 0:
                    pl.when(z == at)(lambda count=count: sent(count, along_send))

        return begin, turn, row_ready, settle

    def swap(block_of, buf, sems):
        def send_row(zz, h):
            for xx in range(nx):
                to = zz * nx + xx

                @pl.when(to != me)
                def _():
                    remote(
                        block_of(to, h), buf.at[h, aligned(me, rows), :], sems[0].at[0], sems[1].at[h], dp=to
                    ).start()

        def ready(h):
            place = buf.at[h, : (n - 1) * rows, :]
            remote(place, place, sems[0].at[0], sems[1].at[h], dp=lax.rem(me + 1, n)).wait_recv()

        def settle():
            place = buf.at[:, : (n - 1) * rows, :]
            remote(place, place, sems[0].at[0], sems[1].at[0], dp=lax.rem(me + 1, n)).wait_send()

        return send_row, ready, settle

    least = jnp.minimum(z, nz - 1 - z)
    longer = jnp.where(z < nz - 1 - z, 1, -1)

    def arriving(r):
        near_turn = r <= 2 * least
        step = jnp.where(near_turn, (r + 1) // 2, r - least)
        sign = jnp.where(near_turn, jnp.where(lax.rem(r, 2) == 1, -1, 1), longer)
        return z + sign * step

    def turn_over(buf, turned, zz):
        turned[:, aligned(zz, span)] = buf[aligned(zz, span), :].T

    def project(buf, gate_weight, up_weight, zz):
        part = aligned(zz, span)
        block = buf[part, :]
        gate_pre[part, :] = jnp.dot(block, gate_weight, preferred_element_type=F32) * scale
        up_pre[part, :] = jnp.dot(block, up_weight, preferred_element_type=F32) * scale

    def activate(cotangent, zz):
        part = aligned(zz, span)
        gate = gate_pre[part, :]
        sigma = jax.nn.sigmoid(gate)
        upstream = cotangent[part, :].astype(F32)
        gate_rows[part, :] = (upstream * up_pre[part, :] * sigma * (1.0 + gate * (1.0 - sigma))).astype(BF16)
        up_rows[part, :] = (upstream * gate * sigma).astype(BF16)

    def update(turned, weight, h, i):
        part = aligned(i, BLOCK)
        block = turned[part, :]
        for s, unit_rows in enumerate((gate_rows, up_rows)):
            gradient = jnp.dot(block, unit_rows[...], preferred_element_type=F32) * scale
            weight[h, s, part, :] = (weight[h, s, part, :].astype(F32) - 0.5 * gradient).astype(BF16)

    def near_copy(h, i):
        place = (h, slice(None), aligned(i, BLOCK))
        return remote(held.at[place], near.at[place], near_sems[0].at[0], near_sems[1].at[h], grp=near_grp)

    def near_slab(h):
        return remote(held.at[h], near.at[h], near_sems[0].at[0], near_sems[1].at[h], grp=near_grp)

    def far_copy(h, i):
        place = (h, slice(None), aligned(i, BLOCK))
        k = jnp.where(h == slabs - 1, h + i, h)
        return remote(held.at[place], far.at[place], far_sems[0].at[0], far_sems[1].at[k], grp=far_grp)

    def far_slab(h):
        return remote(held.at[h], far.at[h], far_sems[0].at[0], far_sems[1].at[h], grp=far_grp)

    def far_sent(first):
        place = pl.ds(first, slabs - first)
        remote(held.at[place], far.at[place], far_sems[0].at[0], far_sems[1].at[0], grp=far_grp).wait_send()

    late = even & (lax.rem(grp // 2, 2) == 1)

    def send_steps(h, i):
        kept = late & (h == slabs - 1) & (i >= blocks // 2)
        pl.when((even & jnp.logical_not(kept)) | (odd & (h > 0)))(lambda: far_copy(h, i).start())
        near_copy(h, i).start()

    @pl.when(odd)
    def _():
        start_early()
        with jax.named_scope("wait_turn"):
            pl.semaphore_wait(turn_sem, 1)

    begin, turn, tokens_ready, settle_tokens = relay(tok, gather_sems)
    send_cot, cot_ready, settle_cot = swap(hidden_part, cot, cot_sems)
    wait_mine(0)
    begin()
    send_cot(z, 0)
    wait_mine(1)
    wait_mine(2)

    @pl.loop(0, nz)
    def _(r):
        pl.when(r < nz - 1)(lambda: turn(r, lambda zz: send_cot(zz, 0)))
        zz = arriving(r)
        with jax.named_scope("wait_side"):
            tokens_ready(zz)
        with jax.named_scope("project"):
            turn_over(tok, tok_t, zz)
            project(tok, held[0, 0], held[0, 1], zz)

    @pl.loop(1, slabs)
    def _(h):
        @pl.loop(0, nz)
        def _(r):
            send_cot(arriving(r), h)

    @pl.loop(0, slabs)
    def _(h):
        @pl.when(h > 0)
        def _():
            @pl.loop(0, nz)
            def _(zz):
                project(tok, held[h, 0], held[h, 1], zz)

        with jax.named_scope("wait_cot"):
            cot_ready(h)

        @pl.loop(0, nz)
        def _(zz):
            with jax.named_scope("forward"):
                activate(cot.at[h], zz)

        @pl.when((h == slabs - 1) & even)
        def _():
            pl.semaphore_signal(turn_sem, inc=1, device_id={"grp": near_grp}, device_id_type=MESH)

        @pl.loop(0, blocks)
        def _(i):
            with jax.named_scope("step"):
                update(tok_t, held, h, i)
            pl.when(i >= 1)(lambda: send_steps(h, i - 1))

        send_steps(h, blocks - 1)

    settle_tokens()
    settle_cot()

    @pl.when(even)
    def _():
        with jax.named_scope("wait_sibling"):
            near_slab(0).wait_recv()
        for copy in early_whole():
            copy.wait_recv()
        begin, turn, tokens_ready, settle_far_tokens = relay(far_tok, gather_sems)
        send_cot, cot_ready, settle_far_cot = swap(
            lambda to, h: stage.at[:, aligned(to, width)], far_cot, cot_sems
        )
        begin()

        @pl.loop(0, nz)
        def _(r):
            send_cot(arriving(r), 0)

        @pl.loop(0, nz)
        def _(r):
            pl.when(r < nz - 1)(lambda: turn(r, lambda zz: None))
            zz = arriving(r)
            with jax.named_scope("wait_side"):
                tokens_ready(zz)
            with jax.named_scope("forward_far"):
                turn_over(far_tok, far_tok_t, zz)
                project(far_tok, far[0, 0], far[0, 1], zz)

        with jax.named_scope("wait_cot"):
            cot_ready(0)

        @pl.loop(0, nz)
        def _(zz):
            activate(far_cot.at[0], zz)

        @pl.loop(0, blocks)
        def _(i):
            with jax.named_scope("step_far"):
                update(far_tok_t, far, 0, i)

        settle_far_tokens()
        settle_far_cot()

    @pl.when(odd)
    def _():
        for copy in early_whole():
            copy.wait_send()

    @pl.loop(0, slabs)
    def _(h):
        with jax.named_scope("wait_near"):
            pl.when(odd | (h > 0))(lambda: near_slab(h).wait_recv())
        pl.when((h < slabs - 1) & (odd | (h > 0)))(lambda: far_slab(h).wait_recv())

        @pl.when(h == slabs - 1)
        def _():
            remote(held, near, near_sems[0].at[0], near_sems[1].at[0], grp=near_grp).wait_send()

        @pl.loop(0, blocks)
        def _(i):
            with jax.named_scope("wait_far"):
                pl.when(h == slabs - 1)(lambda: far_copy(h, i).wait_recv())
            freed = i + blocks // 2 - 1
            pl.when(late & (h == slabs - 1) & (i >= 1) & (freed < blocks))(lambda: far_copy(h, freed).start())
            with jax.named_scope("mix"):
                part = aligned(i, BLOCK)
                for s in range(2):
                    mixed = 0.5 * held[h, s, part, :].astype(F32) + 0.25 * (
                        near[h, s, part, :].astype(F32) + far[h, s, part, :].astype(F32)
                    )
                    far[h, s, part, :] = mixed.astype(BF16)

    pl.when(odd)(lambda: far_sent(1))
    pl.when(even)(lambda: far_sent(0))


def place_kernel(mixed, out_gate, out_up, sems):
    slabs, _, depth, width = mixed.shape
    for part in range(WRITES):
        rows = pl.ds(part * depth // WRITES, depth // WRITES)
        for h in range(slabs):
            for s, out in enumerate((out_gate, out_up)):
                pltpu.make_async_copy(mixed.at[h, s, rows], out.at[rows, pl.ds(h * width, width)], sems.at[0]).start()
    pltpu.make_async_copy(mixed, mixed, sems.at[0]).wait()


def local(tokens, hidden_grad, w_gate, w_up):
    n, groups = lax.axis_size("dp"), lax.axis_size("grp")
    nx = inner_size(n)
    nz = n // nx
    args = [pltpu.with_memory_space_constraint(a[0], pltpu.HBM) for a in (tokens, hidden_grad, w_gate, w_up)]
    rows, depth = args[0].shape
    units = args[2].shape[1]
    total = n * rows
    slabs = slab_count(units)
    width = units // slabs
    blocks = depth // BLOCK
    dma = pltpu.SemaphoreType.DMA
    hops = [dma, dma((nz, PIECES)), dma, dma((nz, max(nx - 1, 1)))]
    weights = (slabs, 2, depth, width)
    scratch = [
        pltpu.VMEM((total, depth), BF16),
        pltpu.VMEM((depth, total), BF16),
        pltpu.VMEM((slabs, total, width), BF16),
        pltpu.VMEM(weights, BF16),
        pltpu.VMEM(weights, BF16),
        pltpu.VMEM((total, depth), BF16),
        pltpu.VMEM((depth, total), BF16),
        pltpu.VMEM((1, total, width), BF16),
        pltpu.VMEM((rows, n * width), BF16),
        pltpu.VMEM((total, width), BF16),
        pltpu.VMEM((total, width), BF16),
        pltpu.VMEM((total, width), F32),
        pltpu.VMEM((total, width), F32),
        dma((3,)), pltpu.SemaphoreType.REGULAR,
        *hops,
        dma((1,)), dma((slabs,)),
        dma((3,)), dma((3,)),
        dma((1,)), dma((slabs,)),
        dma((1,)), dma((slabs - 1 + blocks,)),
    ]
    mixed = pl.pallas_call(
        functools.partial(kernel, n, groups),
        out_shape=pltpu.VMEM(weights, BF16),
        in_specs=[ANY] * 4,
        out_specs=VMEM,
        scratch_shapes=scratch,
        compiler_params=pltpu.CompilerParams(
            collective_id=0, has_side_effects=True, vmem_limit_bytes=VMEM_LIMIT
        ),
        name="gossip_step",
    )(*args)
    shape = jax.ShapeDtypeStruct((depth, units), BF16)
    outs = pl.pallas_call(
        place_kernel,
        out_shape=[shape, shape],
        in_specs=[VMEM],
        out_specs=[ANY] * 2,
        scratch_shapes=[dma((1,))],
        compiler_params=pltpu.CompilerParams(vmem_limit_bytes=8 * 1024 * 1024),
        name="place",
    )(pltpu.with_memory_space_constraint(mixed, pltpu.VMEM))
    return tuple(out[None] for out in outs)


def solution(mesh):
    in_specs = (
        P("grp", "dp", None),
        P("grp", "dp", None),
        P("grp", None, "dp"),
        P("grp", None, "dp"),
    )
    out_specs = (P("grp", None, "dp"), P("grp", None, "dp"))
    return jax.shard_map(local, mesh=mesh, in_specs=in_specs, out_specs=out_specs, check_vma=False)
```

```python
import functools

import jax
import jax.numpy as jnp
from jax import lax
from jax.experimental import pallas as pl
from jax.experimental.pallas import tpu as pltpu
from jax.sharding import PartitionSpec as P

LANES = 128
BLOCK = 256
PIECES = 2
LAG = 2
VMEM_LIMIT = 42 * 1024 * 1024
SMALL_LIMIT = 8 * 1024 * 1024
VMEM = pl.BlockSpec(memory_space=pltpu.VMEM)
ANY = pl.BlockSpec(memory_space=pl.ANY)
MESH = pl.DeviceIdType.MESH
F32, BF16 = jnp.float32, jnp.bfloat16


def inner_size(n):
    return max(d for d in range(1, n + 1) if n % d == 0 and d * d <= n)


def slab_count(units):
    return next(count for count in (3, 2, 1) if units % (count * LANES) == 0)


def closing_rows(depth):
    return (depth // BLOCK - depth // BLOCK // 2) * BLOCK


def aligned(index, size):
    return pl.ds(pl.multiple_of(index * size, size), size)


def roles(groups):
    grp = lax.axis_index("grp")
    odd = lax.rem(grp, 2) == 1
    near_grp = jnp.where(odd, grp - 1, grp + 1)
    far_grp = jnp.where(odd, lax.rem(grp + 1, groups), lax.rem(grp + groups - 1, groups))
    second = lax.rem(jnp.where(odd, far_grp, grp) // 2, 2) == 1
    return odd, near_grp, far_grp, second


def blend(own, near, far):
    return (0.5 * own.astype(F32) + 0.25 * (near.astype(F32) + far.astype(F32))).astype(BF16)


def kernel(n, groups, *refs):
    tokens, hidden, w_gate, w_up, far, held, near = refs[:7]
    tok, tok_t, cot, far_tok, far_tok_t, far_cot, stage, gate_rows, up_rows, gate_pre, up_pre = refs[7:18]
    local_sem, turn_sem = refs[18:20]
    gather_sems = refs[20:24]
    cot_sems, early_sems, near_sems, far_sems = (refs[k : k + 2] for k in range(24, 32, 2))
    nx = inner_size(n)
    nz = n // nx
    rows, depth = tokens.shape
    units = w_gate.shape[1]
    slabs, _, _, width = held.shape
    scale = depth ** (-0.5)
    blocks = depth // BLOCK
    span = nx * rows
    me = lax.axis_index("dp")
    z, x = me // nx, lax.rem(me, nx)
    odd, near_grp, far_grp, second = roles(groups)
    even = jnp.logical_not(odd)

    def hidden_part(to, h):
        return hidden.at[:, pl.ds(pl.multiple_of(to * units + h * width, LANES), width)]

    def wait_mine(k):
        place = (tok.at[aligned(me, rows), :], cot.at[:, aligned(me, rows), :], held)[k]
        pltpu.make_async_copy(place, place, local_sem.at[k]).wait()

    barrier = pltpu.get_barrier_semaphore()

    def greet(**to):
        pl.semaphore_signal(barrier, inc=1, device_id=to, device_id_type=MESH)

    greet(grp=far_grp)
    pl.when(odd)(lambda: greet(grp=near_grp))

    @pl.when(even)
    def _():
        for j in range(1, nx):
            greet(dp=z * nx + lax.rem(x + j, nx))
        pl.when(z >= 1)(lambda: greet(dp=me - nx))
        pl.when(z + 1 < nz)(lambda: greet(dp=me + nx))

    mine = [pltpu.make_async_copy(tokens, tok.at[aligned(me, rows), :], local_sem.at[0])]
    for h in range(slabs):
        mine.append(pltpu.make_async_copy(hidden_part(me, h), cot.at[h, aligned(me, rows), :], local_sem.at[1]))
        for s, w in enumerate((w_gate, w_up)):
            mine.append(pltpu.make_async_copy(w.at[:, pl.ds(h * width, width)], held.at[h, s], local_sem.at[2]))
    for copy in mine:
        copy.start()

    with jax.named_scope("barrier"):
        expected = nx + 1 + jnp.where(z >= 1, 1, 0) + jnp.where(z + 1 < nz, 1, 0)
        pl.semaphore_wait(barrier, jnp.where(odd, 1, expected))

    def remote(src, dst, send, recv, **to):
        return pltpu.make_async_remote_copy(
            src_ref=src, dst_ref=dst, send_sem=send, recv_sem=recv, device_id=to, device_id_type=MESH
        )

    def early(k, src, dst):
        return remote(src, dst, early_sems[0].at[k], early_sems[1].at[k], grp=far_grp)

    def start_early():
        place = aligned(me, rows)
        early(0, tokens, far_tok.at[place, :]).start()
        for s, w in enumerate((w_gate, w_up)):
            early(1, w.at[:, :width], far.at[0, s]).start()
        for j in range(1, n):
            to = lax.rem(me + j, n)
            early(2, hidden_part(to, 0), stage.at[:, aligned(to, width)]).start()
        early(2, hidden_part(me, 0), far_cot.at[0, aligned(me, rows), :]).start()

    def early_whole():
        return [early(k, ref, ref) for k, ref in enumerate((far_tok.at[aligned(me, rows), :], far.at[0], stage))]

    def relay(buf, sems):
        along_send, along_recv, side_send, side_recv = sems
        piece = rows // PIECES

        def slot(zz, xx, c):
            return buf.at[aligned((zz * nx + xx) * PIECES + c, piece), :]

        def along(zz, c, to):
            place = slot(zz, x, c)
            return remote(place, place, along_send, along_recv.at[zz, c], dp=to * nx + x)

        def up(zz, c, back=False):
            return along(zz, c, z - 1 if back else z + 1)

        def down(zz, c, back=False):
            return along(zz, c, z + 1 if back else z - 1)

        def side(zz, j, c):
            place = slot(zz, x, c)
            return remote(place, place, side_send, side_recv.at[zz, j - 1], dp=z * nx + lax.rem(x + j, nx))

        def pass_on(zz, c, upward):
            if upward is not False:
                pl.when(z + 1 < nz)(lambda: up(zz, c).start())
            if upward is not True:
                pl.when(z >= 1)(lambda: down(zz, c).start())
            for j in range(1, nx):
                side(zz, j, c).start()

        def begin():
            for c in range(PIECES):
                pass_on(z, c, None)

        def turn(r, then):
            for c in range(PIECES):
                @pl.when(z - 1 - r >= 0)
                def _():
                    with jax.named_scope("wait_up"):
                        up(z - 1 - r, c, True).wait_recv()
                    pass_on(z - 1 - r, c, True)

                @pl.when(z + 1 + r < nz)
                def _():
                    with jax.named_scope("wait_down"):
                        down(z + 1 + r, c, True).wait_recv()
                    pass_on(z + 1 + r, c, False)

            pl.when(z - 1 - r >= 0)(lambda: then(z - 1 - r))
            pl.when(z + 1 + r < nz)(lambda: then(z + 1 + r))

        def row_ready(zz):
            for j in range(1, nx):
                other = lax.rem(x + nx - j, nx)
                place = buf.at[aligned(zz * nx + other, rows), :]
                remote(place, place, side_send, side_recv.at[zz, j - 1], dp=z * nx + other).wait_recv()

        def settle():
            def sent(count, sem):
                place = buf.at[: count * rows, :]
                remote(place, place, sem, side_recv.at[0, 0], dp=lax.rem(me + 1, n)).wait_send()

            if nx > 1:
                sent(nz * (nx - 1), side_send)
            for at in range(nz):
                count = (at + 1 if at + 1 < nz else 0) + (nz - at if at >= 1 else 0)
                if count > 0:
                    pl.when(z == at)(lambda count=count: sent(count, along_send))

        return begin, turn, row_ready, settle

    def swap(block_of, buf, sems):
        def send_row(zz, h):
            for xx in range(nx):
                to = zz * nx + xx

                @pl.when(to != me)
                def _():
                    remote(
                        block_of(to, h), buf.at[h, aligned(me, rows), :], sems[0].at[0], sems[1].at[h], dp=to
                    ).start()

        def ready(h):
            place = buf.at[h, : (n - 1) * rows, :]
            remote(place, place, sems[0].at[0], sems[1].at[h], dp=lax.rem(me + 1, n)).wait_recv()

        def settle():
            place = buf.at[:, : (n - 1) * rows, :]
            remote(place, place, sems[0].at[0], sems[1].at[0], dp=lax.rem(me + 1, n)).wait_send()

        return send_row, ready, settle

    least = jnp.minimum(z, nz - 1 - z)
    longer = jnp.where(z < nz - 1 - z, 1, -1)

    def arriving(r):
        near_turn = r <= 2 * least
        step = jnp.where(near_turn, (r + 1) // 2, r - least)
        sign = jnp.where(near_turn, jnp.where(lax.rem(r, 2) == 1, -1, 1), longer)
        return z + sign * step

    def turn_over(buf, turned, zz):
        turned[:, aligned(zz, span)] = buf[aligned(zz, span), :].T

    def project(buf, gate_weight, up_weight, zz):
        part = aligned(zz, span)
        block = buf[part, :]
        gate_pre[part, :] = jnp.dot(block, gate_weight, preferred_element_type=F32) * scale
        up_pre[part, :] = jnp.dot(block, up_weight, preferred_element_type=F32) * scale

    def activate(cotangent, zz):
        part = aligned(zz, span)
        gate = gate_pre[part, :]
        sigma = jax.nn.sigmoid(gate)
        upstream = cotangent[part, :].astype(F32)
        gate_rows[part, :] = (upstream * up_pre[part, :] * sigma * (1.0 + gate * (1.0 - sigma))).astype(BF16)
        up_rows[part, :] = (upstream * gate * sigma).astype(BF16)

    def update(turned, weight, h, i):
        part = aligned(i, BLOCK)
        block = turned[part, :]
        for s, unit_rows in enumerate((gate_rows, up_rows)):
            gradient = jnp.dot(block, unit_rows[...], preferred_element_type=F32) * scale
            weight[h, s, part, :] = (weight[h, s, part, :].astype(F32) - 0.5 * gradient).astype(BF16)

    def near_copy(h, i):
        place = (h, slice(None), aligned(i, BLOCK))
        return remote(held.at[place], near.at[place], near_sems[0].at[0], near_sems[1].at[h], grp=near_grp)

    def near_slab(h):
        return remote(held.at[h], near.at[h], near_sems[0].at[0], near_sems[1].at[h], grp=near_grp)

    def far_copy(h, i):
        place = (h, slice(None), aligned(i, BLOCK))
        k = jnp.where(h == slabs - 1, h + i, h)
        last = jnp.where(h == slabs - 1, 1, 0)
        return remote(held.at[place], far.at[place], far_sems[0].at[last], far_sems[1].at[k], grp=far_grp)

    def far_slab(h):
        return remote(held.at[h], far.at[h], far_sems[0].at[0], far_sems[1].at[h], grp=far_grp)

    def far_sent(k, place):
        remote(held.at[place], far.at[place], far_sems[0].at[k], far_sems[1].at[0], grp=far_grp).wait_send()

    kept = blocks // 2

    def send_steps(h, i):
        now = (h < slabs - 1) | (i < kept) | (odd & jnp.logical_not(second))
        pl.when(now & (even | (h > 0)))(lambda: far_copy(h, i).start())
        near_copy(h, i).start()

    @pl.when(odd)
    def _():
        start_early()
        with jax.named_scope("wait_turn"):
            pl.semaphore_wait(turn_sem, 1)

    begin, turn, tokens_ready, settle_tokens = relay(tok, gather_sems)
    send_cot, cot_ready, settle_cot = swap(hidden_part, cot, cot_sems)
    wait_mine(0)
    begin()
    send_cot(z, 0)
    wait_mine(1)
    wait_mine(2)

    @pl.loop(0, nz)
    def _(r):
        pl.when(r < nz - 1)(lambda: turn(r, lambda zz: send_cot(zz, 0)))
        zz = arriving(r)
        with jax.named_scope("wait_side"):
            tokens_ready(zz)
        with jax.named_scope("project"):
            turn_over(tok, tok_t, zz)
            project(tok, held[0, 0], held[0, 1], zz)

    @pl.loop(1, slabs)
    def _(h):
        @pl.loop(0, nz)
        def _(r):
            send_cot(arriving(r), h)

    @pl.loop(0, slabs)
    def _(h):
        @pl.when(h > 0)
        def _():
            @pl.loop(0, nz)
            def _(zz):
                project(tok, held[h, 0], held[h, 1], zz)

        with jax.named_scope("wait_cot"):
            cot_ready(h)

        @pl.loop(0, nz)
        def _(zz):
            with jax.named_scope("forward"):
                activate(cot.at[h], zz)

        @pl.when((h == slabs - 1) & even)
        def _():
            pl.semaphore_signal(turn_sem, inc=1, device_id={"grp": near_grp}, device_id_type=MESH)

        @pl.loop(0, blocks)
        def _(i):
            with jax.named_scope("step"):
                update(tok_t, held, h, i)
            pl.when(i >= 1)(lambda: send_steps(h, i - 1))

        send_steps(h, blocks - 1)

    settle_tokens()
    settle_cot()

    @pl.when(even)
    def _():
        with jax.named_scope("wait_sibling"):
            near_slab(0).wait_recv()
        for copy in early_whole():
            copy.wait_recv()
        begin, turn, tokens_ready, settle_far_tokens = relay(far_tok, gather_sems)
        send_cot, cot_ready, settle_far_cot = swap(
            lambda to, h: stage.at[:, aligned(to, width)], far_cot, cot_sems
        )
        begin()

        @pl.loop(0, nz)
        def _(r):
            send_cot(arriving(r), 0)

        @pl.loop(0, nz)
        def _(r):
            pl.when(r < nz - 1)(lambda: turn(r, lambda zz: None))
            zz = arriving(r)
            with jax.named_scope("wait_side"):
                tokens_ready(zz)
            with jax.named_scope("forward_far"):
                turn_over(far_tok, far_tok_t, zz)
                project(far_tok, far[0, 0], far[0, 1], zz)

        with jax.named_scope("wait_cot"):
            cot_ready(0)

        @pl.loop(0, nz)
        def _(zz):
            activate(far_cot.at[0], zz)

        @pl.loop(0, blocks)
        def _(i):
            with jax.named_scope("step_far"):
                update(far_tok_t, far, 0, i)

        settle_far_tokens()
        settle_far_cot()

    @pl.when(odd)
    def _():
        for copy in early_whole():
            copy.wait_send()

    @pl.loop(0, slabs)
    def _(h):
        with jax.named_scope("wait_near"):
            pl.when(odd | (h > 0))(lambda: near_slab(h).wait_recv())
        pl.when((h < slabs - 1) & (odd | (h > 0)))(lambda: far_slab(h).wait_recv())

        @pl.when(h == slabs - 1)
        def _():
            remote(held, near, near_sems[0].at[0], near_sems[1].at[0], grp=near_grp).wait_send()

        @pl.loop(0, jnp.where(second & (h == slabs - 1), kept, blocks))
        def _(i):
            with jax.named_scope("wait_far"):
                pl.when(h == slabs - 1)(lambda: far_copy(h, i).wait_recv())
            freed = i + kept - LAG
            behind = even & jnp.logical_not(second) & (h == slabs - 1)
            pl.when(behind & (freed >= kept) & (freed < blocks))(lambda: far_copy(h, freed).start())
            with jax.named_scope("mix"):
                part = aligned(i, BLOCK)
                for s in range(2):
                    far[h, s, part, :] = blend(held[h, s, part, :], near[h, s, part, :], far[h, s, part, :])

    pl.when(odd)(lambda: far_sent(0, pl.ds(1, slabs - 2)))
    pl.when(even)(lambda: far_sent(0, pl.ds(0, slabs - 1)))
    pl.when(second)(lambda: far_sent(1, (slabs - 1, slice(None), pl.ds(0, kept * BLOCK))))
    pl.when(jnp.logical_not(second))(lambda: far_sent(1, slabs - 1))


def closing_kernel(groups, mixed, held, near, placed, tail, send_sem, recv_sem):
    _, _, far_grp, second = roles(groups)
    last = held.shape[0] - 1
    depth = tail.shape[1]
    start = held.shape[2] - depth

    @pl.when(second)
    def _():
        barrier = pltpu.get_barrier_semaphore()
        pl.semaphore_signal(barrier, inc=1, device_id={"grp": far_grp}, device_id_type=MESH)
        pl.semaphore_wait(barrier, 1)

        def copy(i):
            return pltpu.make_async_remote_copy(
                src_ref=held.at[last, :, pl.ds(pl.multiple_of(start + i * BLOCK, BLOCK), BLOCK)],
                dst_ref=tail.at[:, aligned(i, BLOCK)], send_sem=send_sem.at[0], recv_sem=recv_sem.at[i],
                device_id={"grp": far_grp}, device_id_type=MESH,
            )

        @pl.loop(0, depth // BLOCK)
        def _(i):
            copy(i).start()

        @pl.loop(0, depth // BLOCK)
        def _(i):
            with jax.named_scope("wait_tail"):
                copy(i).wait_recv()
            part = aligned(i, BLOCK)
            rows = pl.ds(pl.multiple_of(start + i * BLOCK, BLOCK), BLOCK)
            for s in range(2):
                tail[s, part, :] = blend(held[last, s, rows, :], near[last, s, rows, :], tail[s, part, :])

        pltpu.make_async_remote_copy(
            src_ref=tail, dst_ref=tail, send_sem=send_sem.at[0], recv_sem=recv_sem.at[0],
            device_id={"grp": far_grp}, device_id_type=MESH,
        ).wait_send()

    @pl.when(jnp.logical_not(second))
    def _():
        for s in range(2):
            tail[s] = mixed[last, s, start:, :]


def place_kernel(mixed, out_gate, out_up, sems):
    slabs, _, depth, width = mixed.shape
    copies = []
    for h in range(slabs):
        step = depth // 4
        for start in range(0, depth if h < slabs - 1 else depth - closing_rows(depth), step):
            for s, out in enumerate((out_gate, out_up)):
                rows = pl.ds(start, step)
                copies.append(
                    pltpu.make_async_copy(mixed.at[h, s, rows], out.at[rows, pl.ds(h * width, width)], sems.at[len(copies)])
                )
    for copy in copies:
        copy.start()
    for copy in copies:
        copy.wait()


def place_tail_kernel(tail, held_gate, held_up, out_gate, out_up, sems):
    _, rows, width = tail.shape
    depth, units = out_gate.shape
    step = rows // 2
    copies = [
        pltpu.make_async_copy(
            tail.at[s, pl.ds(k * step, step)],
            out.at[pl.ds(depth - rows + k * step, step), pl.ds(units - width, width)], sems.at[s, k],
        )
        for s, out in enumerate((out_gate, out_up))
        for k in range(2)
    ]
    for copy in copies:
        copy.start()
    for copy in copies:
        copy.wait()


def local(tokens, hidden_grad, w_gate, w_up):
    n, groups = lax.axis_size("dp"), lax.axis_size("grp")
    nx = inner_size(n)
    nz = n // nx
    args = [pltpu.with_memory_space_constraint(a[0], pltpu.HBM) for a in (tokens, hidden_grad, w_gate, w_up)]
    rows, depth = args[0].shape
    units = args[2].shape[1]
    total = n * rows
    slabs = slab_count(units)
    width = units // slabs
    blocks = depth // BLOCK
    dma = pltpu.SemaphoreType.DMA
    hops = [dma, dma((nz, PIECES)), dma, dma((nz, max(nx - 1, 1)))]
    weights = (slabs, 2, depth, width)
    scratch = [
        pltpu.VMEM((total, depth), BF16),
        pltpu.VMEM((depth, total), BF16),
        pltpu.VMEM((slabs, total, width), BF16),
        pltpu.VMEM((total, depth), BF16),
        pltpu.VMEM((depth, total), BF16),
        pltpu.VMEM((1, total, width), BF16),
        pltpu.VMEM((rows, n * width), BF16),
        pltpu.VMEM((total, width), BF16),
        pltpu.VMEM((total, width), BF16),
        pltpu.VMEM((total, width), F32),
        pltpu.VMEM((total, width), F32),
        dma((3,)), pltpu.SemaphoreType.REGULAR,
        *hops,
        dma((1,)), dma((slabs,)),
        dma((3,)), dma((3,)),
        dma((1,)), dma((slabs,)),
        dma((2,)), dma((slabs - 1 + blocks,)),
    ]
    kept = pltpu.VMEM(weights, BF16)
    mixed, held, near = pl.pallas_call(
        functools.partial(kernel, n, groups),
        out_shape=[kept, kept, kept],
        in_specs=[ANY] * 4,
        out_specs=[VMEM] * 3,
        scratch_shapes=scratch,
        compiler_params=pltpu.CompilerParams(
            collective_id=0, has_side_effects=True, vmem_limit_bytes=VMEM_LIMIT
        ),
        name="gossip_step",
    )(*args)
    mixed, held, near = (pltpu.with_memory_space_constraint(a, pltpu.VMEM) for a in (mixed, held, near))
    shape = jax.ShapeDtypeStruct((depth, units), BF16)
    outs = pl.pallas_call(
        place_kernel,
        out_shape=[shape, shape],
        in_specs=[VMEM],
        out_specs=[ANY] * 2,
        scratch_shapes=[dma((8 * slabs,))],
        compiler_params=pltpu.CompilerParams(vmem_limit_bytes=SMALL_LIMIT),
        name="place",
    )(mixed)
    tail_rows = closing_rows(depth)
    tail = pl.pallas_call(
        functools.partial(closing_kernel, groups),
        out_shape=pltpu.VMEM((2, tail_rows, width), BF16),
        in_specs=[VMEM] * 3 + [ANY],
        out_specs=VMEM,
        scratch_shapes=[dma((1,)), dma((tail_rows // BLOCK,))],
        compiler_params=pltpu.CompilerParams(
            collective_id=1, has_side_effects=True, vmem_limit_bytes=SMALL_LIMIT
        ),
        name="closing",
    )(mixed, held, near, pltpu.with_memory_space_constraint(outs[0], pltpu.HBM))
    outs = pl.pallas_call(
        place_tail_kernel,
        out_shape=[shape, shape],
        in_specs=[VMEM, ANY, ANY],
        out_specs=[ANY] * 2,
        input_output_aliases={1: 0, 2: 1},
        scratch_shapes=[dma((2, 2))],
        compiler_params=pltpu.CompilerParams(vmem_limit_bytes=SMALL_LIMIT),
        name="place_tail",
    )(
        pltpu.with_memory_space_constraint(tail, pltpu.VMEM),
        *(pltpu.with_memory_space_constraint(out, pltpu.HBM) for out in outs),
    )
    return tuple(out[None] for out in outs)


def solution(mesh):
    in_specs = (
        P("grp", "dp", None),
        P("grp", "dp", None),
        P("grp", None, "dp"),
        P("grp", None, "dp"),
    )
    out_specs = (P("grp", None, "dp"), P("grp", None, "dp"))
    return jax.shard_map(local, mesh=mesh, in_specs=in_specs, out_specs=out_specs, check_vma=False)
```

```python
import functools

import jax
import jax.numpy as jnp
from jax import lax
from jax.experimental import pallas as pl
from jax.experimental.pallas import tpu as pltpu
from jax.sharding import PartitionSpec as P

LANES = 128
BLOCK = 256
PIECES = 2
LAG = 2
VMEM_LIMIT = 42 * 1024 * 1024
SMALL_LIMIT = 8 * 1024 * 1024
VMEM = pl.BlockSpec(memory_space=pltpu.VMEM)
ANY = pl.BlockSpec(memory_space=pl.ANY)
MESH = pl.DeviceIdType.MESH
F32, BF16 = jnp.float32, jnp.bfloat16


def inner_size(n):
    return max(d for d in range(1, n + 1) if n % d == 0 and d * d <= n)


def slab_count(units):
    return next(count for count in (3, 2, 1) if units % (count * LANES) == 0)


def closing_rows(depth):
    return (depth // BLOCK - depth // BLOCK // 2) * BLOCK


def aligned(index, size):
    return pl.ds(pl.multiple_of(index * size, size), size)


def roles(groups):
    grp = lax.axis_index("grp")
    odd = lax.rem(grp, 2) == 1
    near_grp = jnp.where(odd, grp - 1, grp + 1)
    far_grp = jnp.where(odd, lax.rem(grp + 1, groups), lax.rem(grp + groups - 1, groups))
    second = lax.rem(jnp.where(odd, far_grp, grp) // 2, 2) == 1
    return odd, near_grp, far_grp, second


def blend(own, near, far):
    return (0.5 * own.astype(F32) + 0.25 * (near.astype(F32) + far.astype(F32))).astype(BF16)


def kernel(n, groups, *refs):
    tokens, hidden, w_gate, w_up, far, held, near = refs[:7]
    tok, tok_t, cot, far_tok, far_tok_t, far_cot, stage, gate_rows, up_rows, gate_pre, up_pre = refs[7:18]
    local_sem, turn_sem = refs[18:20]
    gather_sems = refs[20:24]
    cot_sems, early_sems, near_sems, far_sems = (refs[k : k + 2] for k in range(24, 32, 2))
    nx = inner_size(n)
    nz = n // nx
    rows, depth = tokens.shape
    units = w_gate.shape[1]
    slabs, _, _, width = held.shape
    scale = depth ** (-0.5)
    blocks = depth // BLOCK
    span = nx * rows
    me = lax.axis_index("dp")
    z, x = me // nx, lax.rem(me, nx)
    odd, near_grp, far_grp, second = roles(groups)
    even = jnp.logical_not(odd)

    def hidden_part(to, h):
        return hidden.at[:, pl.ds(pl.multiple_of(to * units + h * width, LANES), width)]

    def wait_mine(k):
        place = (tok.at[aligned(me, rows), :], cot.at[:, aligned(me, rows), :], held)[k]
        pltpu.make_async_copy(place, place, local_sem.at[k]).wait()

    barrier = pltpu.get_barrier_semaphore()

    def greet(**to):
        pl.semaphore_signal(barrier, inc=1, device_id=to, device_id_type=MESH)

    greet(grp=far_grp)
    pl.when(odd)(lambda: greet(grp=near_grp))

    @pl.when(even)
    def _():
        for j in range(1, nx):
            greet(dp=z * nx + lax.rem(x + j, nx))
        pl.when(z >= 1)(lambda: greet(dp=me - nx))
        pl.when(z + 1 < nz)(lambda: greet(dp=me + nx))

    mine = [pltpu.make_async_copy(tokens, tok.at[aligned(me, rows), :], local_sem.at[0])]
    for h in range(slabs):
        mine.append(pltpu.make_async_copy(hidden_part(me, h), cot.at[h, aligned(me, rows), :], local_sem.at[1]))
        for s, w in enumerate((w_gate, w_up)):
            mine.append(pltpu.make_async_copy(w.at[:, pl.ds(h * width, width)], held.at[h, s], local_sem.at[2]))
    pl.when(even)(lambda: mine[0].start())

    with jax.named_scope("barrier"):
        expected = nx + 1 + jnp.where(z >= 1, 1, 0) + jnp.where(z + 1 < nz, 1, 0)
        pl.semaphore_wait(barrier, jnp.where(odd, 1, expected))

    def remote(src, dst, send, recv, **to):
        return pltpu.make_async_remote_copy(
            src_ref=src, dst_ref=dst, send_sem=send, recv_sem=recv, device_id=to, device_id_type=MESH
        )

    def early(k, src, dst):
        return remote(src, dst, early_sems[0].at[k], early_sems[1].at[k], grp=far_grp)

    def start_early():
        place = aligned(me, rows)
        early(0, tokens, far_tok.at[place, :]).start()
        for s, w in enumerate((w_gate, w_up)):
            early(1, w.at[:, :width], far.at[0, s]).start()
        for j in range(1, n):
            to = lax.rem(me + j, n)
            early(2, hidden_part(to, 0), stage.at[:, aligned(to, width)]).start()
        early(2, hidden_part(me, 0), far_cot.at[0, aligned(me, rows), :]).start()

    def early_whole():
        return [early(k, ref, ref) for k, ref in enumerate((far_tok.at[aligned(me, rows), :], far.at[0], stage))]

    def relay(buf, sems):
        along_send, along_recv, side_send, side_recv = sems
        piece = rows // PIECES

        def slot(zz, xx, c):
            return buf.at[aligned((zz * nx + xx) * PIECES + c, piece), :]

        def along(zz, c, to):
            place = slot(zz, x, c)
            return remote(place, place, along_send, along_recv.at[zz, c], dp=to * nx + x)

        def up(zz, c, back=False):
            return along(zz, c, z - 1 if back else z + 1)

        def down(zz, c, back=False):
            return along(zz, c, z + 1 if back else z - 1)

        def side(zz, j, c):
            place = slot(zz, x, c)
            return remote(place, place, side_send, side_recv.at[zz, j - 1], dp=z * nx + lax.rem(x + j, nx))

        def pass_on(zz, c, upward):
            if upward is not False:
                pl.when(z + 1 < nz)(lambda: up(zz, c).start())
            if upward is not True:
                pl.when(z >= 1)(lambda: down(zz, c).start())
            for j in range(1, nx):
                side(zz, j, c).start()

        def begin():
            for c in range(PIECES):
                pass_on(z, c, None)

        def turn(r, then):
            for c in range(PIECES):
                @pl.when(z - 1 - r >= 0)
                def _():
                    with jax.named_scope("wait_up"):
                        up(z - 1 - r, c, True).wait_recv()
                    pass_on(z - 1 - r, c, True)

                @pl.when(z + 1 + r < nz)
                def _():
                    with jax.named_scope("wait_down"):
                        down(z + 1 + r, c, True).wait_recv()
                    pass_on(z + 1 + r, c, False)

            pl.when(z - 1 - r >= 0)(lambda: then(z - 1 - r))
            pl.when(z + 1 + r < nz)(lambda: then(z + 1 + r))

        def row_ready(zz):
            for j in range(1, nx):
                other = lax.rem(x + nx - j, nx)
                place = buf.at[aligned(zz * nx + other, rows), :]
                remote(place, place, side_send, side_recv.at[zz, j - 1], dp=z * nx + other).wait_recv()

        def settle():
            def sent(count, sem):
                place = buf.at[: count * rows, :]
                remote(place, place, sem, side_recv.at[0, 0], dp=lax.rem(me + 1, n)).wait_send()

            if nx > 1:
                sent(nz * (nx - 1), side_send)
            for at in range(nz):
                count = (at + 1 if at + 1 < nz else 0) + (nz - at if at >= 1 else 0)
                if count > 0:
                    pl.when(z == at)(lambda count=count: sent(count, along_send))

        return begin, turn, row_ready, settle

    def swap(block_of, buf, sems):
        def send_row(zz, h):
            for xx in range(nx):
                to = zz * nx + xx

                @pl.when(to != me)
                def _():
                    remote(
                        block_of(to, h), buf.at[h, aligned(me, rows), :], sems[0].at[0], sems[1].at[h], dp=to
                    ).start()

        def ready(h):
            place = buf.at[h, : (n - 1) * rows, :]
            remote(place, place, sems[0].at[0], sems[1].at[h], dp=lax.rem(me + 1, n)).wait_recv()

        def settle():
            place = buf.at[:, : (n - 1) * rows, :]
            remote(place, place, sems[0].at[0], sems[1].at[0], dp=lax.rem(me + 1, n)).wait_send()

        return send_row, ready, settle

    least = jnp.minimum(z, nz - 1 - z)
    longer = jnp.where(z < nz - 1 - z, 1, -1)

    def arriving(r):
        near_turn = r <= 2 * least
        step = jnp.where(near_turn, (r + 1) // 2, r - least)
        sign = jnp.where(near_turn, jnp.where(lax.rem(r, 2) == 1, -1, 1), longer)
        return z + sign * step

    def turn_over(buf, turned, zz):
        turned[:, aligned(zz, span)] = buf[aligned(zz, span), :].T

    def project(buf, gate_weight, up_weight, zz):
        part = aligned(zz, span)
        block = buf[part, :]
        gate_pre[part, :] = jnp.dot(block, gate_weight, preferred_element_type=F32) * scale
        up_pre[part, :] = jnp.dot(block, up_weight, preferred_element_type=F32) * scale

    def activate(cotangent, zz):
        part = aligned(zz, span)
        gate = gate_pre[part, :]
        sigma = jax.nn.sigmoid(gate)
        upstream = cotangent[part, :].astype(F32)
        gate_rows[part, :] = (upstream * up_pre[part, :] * sigma * (1.0 + gate * (1.0 - sigma))).astype(BF16)
        up_rows[part, :] = (upstream * gate * sigma).astype(BF16)

    def update(turned, weight, h, i):
        part = aligned(i, BLOCK)
        block = turned[part, :]
        for s, unit_rows in enumerate((gate_rows, up_rows)):
            gradient = jnp.dot(block, unit_rows[...], preferred_element_type=F32) * scale
            weight[h, s, part, :] = (weight[h, s, part, :].astype(F32) - 0.5 * gradient).astype(BF16)

    def near_copy(h, i):
        place = (h, slice(None), aligned(i, BLOCK))
        return remote(held.at[place], near.at[place], near_sems[0].at[0], near_sems[1].at[h], grp=near_grp)

    def near_slab(h):
        return remote(held.at[h], near.at[h], near_sems[0].at[0], near_sems[1].at[h], grp=near_grp)

    def far_copy(h, i):
        place = (h, slice(None), aligned(i, BLOCK))
        k = jnp.where(h == slabs - 1, h + i, h)
        last = jnp.where(h == slabs - 1, 1, 0)
        return remote(held.at[place], far.at[place], far_sems[0].at[last], far_sems[1].at[k], grp=far_grp)

    def far_slab(h):
        return remote(held.at[h], far.at[h], far_sems[0].at[0], far_sems[1].at[h], grp=far_grp)

    def far_sent(k, place):
        remote(held.at[place], far.at[place], far_sems[0].at[k], far_sems[1].at[0], grp=far_grp).wait_send()

    kept = blocks // 2

    def send_steps(h, i):
        now = (h < slabs - 1) | (i < kept) | (odd & jnp.logical_not(second))
        pl.when(now & (even | (h > 0)))(lambda: far_copy(h, i).start())
        near_copy(h, i).start()

    @pl.when(odd)
    def _():
        start_early()
        mine[0].start()
        with jax.named_scope("wait_turn"):
            pl.semaphore_wait(turn_sem, 1)

    begin, turn, tokens_ready, settle_tokens = relay(tok, gather_sems)
    send_cot, cot_ready, settle_cot = swap(hidden_part, cot, cot_sems)
    wait_mine(0)
    begin()
    for copy in mine[1:]:
        copy.start()
    send_cot(z, 0)
    wait_mine(1)
    wait_mine(2)

    @pl.loop(0, nz)
    def _(r):
        pl.when(r < nz - 1)(lambda: turn(r, lambda zz: send_cot(zz, 0)))
        zz = arriving(r)
        with jax.named_scope("wait_side"):
            tokens_ready(zz)
        with jax.named_scope("project"):
            turn_over(tok, tok_t, zz)
            project(tok, held[0, 0], held[0, 1], zz)

    @pl.loop(1, slabs)
    def _(h):
        @pl.loop(0, nz)
        def _(r):
            send_cot(arriving(r), h)

    @pl.loop(0, slabs)
    def _(h):
        @pl.when(h > 0)
        def _():
            @pl.loop(0, nz)
            def _(zz):
                project(tok, held[h, 0], held[h, 1], zz)

        with jax.named_scope("wait_cot"):
            cot_ready(h)

        @pl.loop(0, nz)
        def _(zz):
            with jax.named_scope("forward"):
                activate(cot.at[h], zz)

        @pl.when((h == slabs - 1) & even)
        def _():
            pl.semaphore_signal(turn_sem, inc=1, device_id={"grp": near_grp}, device_id_type=MESH)

        @pl.loop(0, blocks)
        def _(i):
            with jax.named_scope("step"):
                update(tok_t, held, h, i)
            pl.when(i >= 1)(lambda: send_steps(h, i - 1))

        send_steps(h, blocks - 1)

    settle_tokens()
    settle_cot()

    @pl.when(even)
    def _():
        with jax.named_scope("wait_sibling"):
            near_slab(0).wait_recv()
        for copy in early_whole():
            copy.wait_recv()
        begin, turn, tokens_ready, settle_far_tokens = relay(far_tok, gather_sems)
        send_cot, cot_ready, settle_far_cot = swap(
            lambda to, h: stage.at[:, aligned(to, width)], far_cot, cot_sems
        )
        begin()

        @pl.loop(0, nz)
        def _(r):
            send_cot(arriving(r), 0)

        @pl.loop(0, nz)
        def _(r):
            pl.when(r < nz - 1)(lambda: turn(r, lambda zz: None))
            zz = arriving(r)
            with jax.named_scope("wait_side"):
                tokens_ready(zz)
            with jax.named_scope("forward_far"):
                turn_over(far_tok, far_tok_t, zz)
                project(far_tok, far[0, 0], far[0, 1], zz)

        with jax.named_scope("wait_cot"):
            cot_ready(0)

        @pl.loop(0, nz)
        def _(zz):
            activate(far_cot.at[0], zz)

        @pl.loop(0, blocks)
        def _(i):
            with jax.named_scope("step_far"):
                update(far_tok_t, far, 0, i)

        settle_far_tokens()
        settle_far_cot()

    @pl.when(odd)
    def _():
        for copy in early_whole():
            copy.wait_send()

    @pl.loop(0, slabs)
    def _(h):
        with jax.named_scope("wait_near"):
            pl.when(odd | (h > 0))(lambda: near_slab(h).wait_recv())
        pl.when((h < slabs - 1) & (odd | (h > 0)))(lambda: far_slab(h).wait_recv())

        @pl.when(h == slabs - 1)
        def _():
            remote(held, near, near_sems[0].at[0], near_sems[1].at[0], grp=near_grp).wait_send()

        @pl.loop(0, jnp.where(second & (h == slabs - 1), kept, blocks))
        def _(i):
            with jax.named_scope("wait_far"):
                pl.when(h == slabs - 1)(lambda: far_copy(h, i).wait_recv())
            freed = i + kept - LAG
            behind = even & jnp.logical_not(second) & (h == slabs - 1)
            pl.when(behind & (freed >= kept) & (freed < blocks))(lambda: far_copy(h, freed).start())
            with jax.named_scope("mix"):
                part = aligned(i, BLOCK)
                for s in range(2):
                    far[h, s, part, :] = blend(held[h, s, part, :], near[h, s, part, :], far[h, s, part, :])

    pl.when(odd)(lambda: far_sent(0, pl.ds(1, slabs - 2)))
    pl.when(even)(lambda: far_sent(0, pl.ds(0, slabs - 1)))
    pl.when(second)(lambda: far_sent(1, (slabs - 1, slice(None), pl.ds(0, kept * BLOCK))))
    pl.when(jnp.logical_not(second))(lambda: far_sent(1, slabs - 1))


def closing_kernel(groups, mixed, held, near, placed, tail, send_sem, recv_sem):
    _, _, far_grp, second = roles(groups)
    last = held.shape[0] - 1
    depth = tail.shape[1]
    start = held.shape[2] - depth

    @pl.when(second)
    def _():
        barrier = pltpu.get_barrier_semaphore()
        pl.semaphore_signal(barrier, inc=1, device_id={"grp": far_grp}, device_id_type=MESH)
        pl.semaphore_wait(barrier, 1)

        def copy(i):
            return pltpu.make_async_remote_copy(
                src_ref=held.at[last, :, pl.ds(pl.multiple_of(start + i * BLOCK, BLOCK), BLOCK)],
                dst_ref=tail.at[:, aligned(i, BLOCK)], send_sem=send_sem.at[0], recv_sem=recv_sem.at[i],
                device_id={"grp": far_grp}, device_id_type=MESH,
            )

        @pl.loop(0, depth // BLOCK)
        def _(i):
            copy(i).start()

        @pl.loop(0, depth // BLOCK)
        def _(i):
            with jax.named_scope("wait_tail"):
                copy(i).wait_recv()
            part = aligned(i, BLOCK)
            rows = pl.ds(pl.multiple_of(start + i * BLOCK, BLOCK), BLOCK)
            for s in range(2):
                tail[s, part, :] = blend(held[last, s, rows, :], near[last, s, rows, :], tail[s, part, :])

        pltpu.make_async_remote_copy(
            src_ref=tail, dst_ref=tail, send_sem=send_sem.at[0], recv_sem=recv_sem.at[0],
            device_id={"grp": far_grp}, device_id_type=MESH,
        ).wait_send()

    @pl.when(jnp.logical_not(second))
    def _():
        for s in range(2):
            tail[s] = mixed[last, s, start:, :]


def place_kernel(mixed, out_gate, out_up, sems):
    slabs, _, depth, width = mixed.shape
    copies = []
    for h in range(slabs):
        step = depth // 4
        for start in range(0, depth if h < slabs - 1 else depth - closing_rows(depth), step):
            for s, out in enumerate((out_gate, out_up)):
                rows = pl.ds(start, step)
                copies.append(
                    pltpu.make_async_copy(mixed.at[h, s, rows], out.at[rows, pl.ds(h * width, width)], sems.at[len(copies)])
                )
    for copy in copies:
        copy.start()
    for copy in copies:
        copy.wait()


def place_tail_kernel(tail, held_gate, held_up, out_gate, out_up, sems):
    _, rows, width = tail.shape
    depth, units = out_gate.shape
    step = rows // 2
    copies = [
        pltpu.make_async_copy(
            tail.at[s, pl.ds(k * step, step)],
            out.at[pl.ds(depth - rows + k * step, step), pl.ds(units - width, width)], sems.at[s, k],
        )
        for s, out in enumerate((out_gate, out_up))
        for k in range(2)
    ]
    for copy in copies:
        copy.start()
    for copy in copies:
        copy.wait()


def local(tokens, hidden_grad, w_gate, w_up):
    n, groups = lax.axis_size("dp"), lax.axis_size("grp")
    nx = inner_size(n)
    nz = n // nx
    args = [pltpu.with_memory_space_constraint(a[0], pltpu.HBM) for a in (tokens, hidden_grad, w_gate, w_up)]
    rows, depth = args[0].shape
    units = args[2].shape[1]
    total = n * rows
    slabs = slab_count(units)
    width = units // slabs
    blocks = depth // BLOCK
    dma = pltpu.SemaphoreType.DMA
    hops = [dma, dma((nz, PIECES)), dma, dma((nz, max(nx - 1, 1)))]
    weights = (slabs, 2, depth, width)
    scratch = [
        pltpu.VMEM((total, depth), BF16),
        pltpu.VMEM((depth, total), BF16),
        pltpu.VMEM((slabs, total, width), BF16),
        pltpu.VMEM((total, depth), BF16),
        pltpu.VMEM((depth, total), BF16),
        pltpu.VMEM((1, total, width), BF16),
        pltpu.VMEM((rows, n * width), BF16),
        pltpu.VMEM((total, width), BF16),
        pltpu.VMEM((total, width), BF16),
        pltpu.VMEM((total, width), F32),
        pltpu.VMEM((total, width), F32),
        dma((3,)), pltpu.SemaphoreType.REGULAR,
        *hops,
        dma((1,)), dma((slabs,)),
        dma((3,)), dma((3,)),
        dma((1,)), dma((slabs,)),
        dma((2,)), dma((slabs - 1 + blocks,)),
    ]
    kept = pltpu.VMEM(weights, BF16)
    mixed, held, near = pl.pallas_call(
        functools.partial(kernel, n, groups),
        out_shape=[kept, kept, kept],
        in_specs=[ANY] * 4,
        out_specs=[VMEM] * 3,
        scratch_shapes=scratch,
        compiler_params=pltpu.CompilerParams(
            collective_id=0, has_side_effects=True, vmem_limit_bytes=VMEM_LIMIT
        ),
        name="gossip_step",
    )(*args)
    mixed, held, near = (pltpu.with_memory_space_constraint(a, pltpu.VMEM) for a in (mixed, held, near))
    shape = jax.ShapeDtypeStruct((depth, units), BF16)
    outs = pl.pallas_call(
        place_kernel,
        out_shape=[shape, shape],
        in_specs=[VMEM],
        out_specs=[ANY] * 2,
        scratch_shapes=[dma((8 * slabs,))],
        compiler_params=pltpu.CompilerParams(vmem_limit_bytes=SMALL_LIMIT),
        name="place",
    )(mixed)
    tail_rows = closing_rows(depth)
    tail = pl.pallas_call(
        functools.partial(closing_kernel, groups),
        out_shape=pltpu.VMEM((2, tail_rows, width), BF16),
        in_specs=[VMEM] * 3 + [ANY],
        out_specs=VMEM,
        scratch_shapes=[dma((1,)), dma((tail_rows // BLOCK,))],
        compiler_params=pltpu.CompilerParams(
            collective_id=1, has_side_effects=True, vmem_limit_bytes=SMALL_LIMIT
        ),
        name="closing",
    )(mixed, held, near, pltpu.with_memory_space_constraint(outs[0], pltpu.HBM))
    outs = pl.pallas_call(
        place_tail_kernel,
        out_shape=[shape, shape],
        in_specs=[VMEM, ANY, ANY],
        out_specs=[ANY] * 2,
        input_output_aliases={1: 0, 2: 1},
        scratch_shapes=[dma((2, 2))],
        compiler_params=pltpu.CompilerParams(vmem_limit_bytes=SMALL_LIMIT),
        name="place_tail",
    )(
        pltpu.with_memory_space_constraint(tail, pltpu.VMEM),
        *(pltpu.with_memory_space_constraint(out, pltpu.HBM) for out in outs),
    )
    return tuple(out[None] for out in outs)


def solution(mesh):
    in_specs = (
        P("grp", "dp", None),
        P("grp", "dp", None),
        P("grp", None, "dp"),
        P("grp", None, "dp"),
    )
    out_specs = (P("grp", None, "dp"), P("grp", None, "dp"))
    return jax.shard_map(local, mesh=mesh, in_specs=in_specs, out_specs=out_specs, check_vma=False)
```

```python
import functools

import jax
import jax.numpy as jnp
from jax import lax
from jax.experimental import pallas as pl
from jax.experimental.pallas import tpu as pltpu
from jax.sharding import PartitionSpec as P

LANES = 128
BLOCK = 256
PIECES = 2
LAG = 1
VMEM_LIMIT = 42 * 1024 * 1024
SMALL_LIMIT = 8 * 1024 * 1024
VMEM = pl.BlockSpec(memory_space=pltpu.VMEM)
ANY = pl.BlockSpec(memory_space=pl.ANY)
MESH = pl.DeviceIdType.MESH
F32, BF16 = jnp.float32, jnp.bfloat16


def inner_size(n):
    return max(d for d in range(1, n + 1) if n % d == 0 and d * d <= n)


def slab_count(units):
    return next(count for count in (3, 2, 1) if units % (count * LANES) == 0)


def closing_rows(depth):
    return (depth // BLOCK - depth // BLOCK // 2) * BLOCK


def aligned(index, size):
    return pl.ds(pl.multiple_of(index * size, size), size)


def roles(groups):
    grp = lax.axis_index("grp")
    odd = lax.rem(grp, 2) == 1
    near_grp = jnp.where(odd, grp - 1, grp + 1)
    far_grp = jnp.where(odd, lax.rem(grp + 1, groups), lax.rem(grp + groups - 1, groups))
    second = lax.rem(jnp.where(odd, far_grp, grp) // 2, 2) == 1
    return odd, near_grp, far_grp, second


def blend(own, near, far):
    return (0.5 * own.astype(F32) + 0.25 * (near.astype(F32) + far.astype(F32))).astype(BF16)


def kernel(n, groups, *refs):
    tokens, hidden, w_gate, w_up, far, held, near = refs[:7]
    tok, tok_t, cot, far_tok, far_tok_t, far_cot, stage, gate_rows, up_rows, gate_pre, up_pre = refs[7:18]
    local_sem, turn_sem = refs[18:20]
    gather_sems = refs[20:24]
    cot_sems, early_sems, near_sems, far_sems = (refs[k : k + 2] for k in range(24, 32, 2))
    nx = inner_size(n)
    nz = n // nx
    rows, depth = tokens.shape
    units = w_gate.shape[1]
    slabs, _, _, width = held.shape
    scale = depth ** (-0.5)
    blocks = depth // BLOCK
    span = nx * rows
    me = lax.axis_index("dp")
    z, x = me // nx, lax.rem(me, nx)
    odd, near_grp, far_grp, second = roles(groups)
    even = jnp.logical_not(odd)

    def hidden_part(to, h):
        return hidden.at[:, pl.ds(pl.multiple_of(to * units + h * width, LANES), width)]

    def wait_mine(k):
        place = (tok.at[aligned(me, rows), :], cot.at[:, aligned(me, rows), :], held)[k]
        pltpu.make_async_copy(place, place, local_sem.at[k]).wait()

    barrier = pltpu.get_barrier_semaphore()

    def greet(**to):
        pl.semaphore_signal(barrier, inc=1, device_id=to, device_id_type=MESH)

    greet(grp=far_grp)
    pl.when(odd)(lambda: greet(grp=near_grp))

    @pl.when(even)
    def _():
        for j in range(1, nx):
            greet(dp=z * nx + lax.rem(x + j, nx))
        pl.when(z >= 1)(lambda: greet(dp=me - nx))
        pl.when(z + 1 < nz)(lambda: greet(dp=me + nx))

    mine = [pltpu.make_async_copy(tokens, tok.at[aligned(me, rows), :], local_sem.at[0])]
    for h in range(slabs):
        mine.append(pltpu.make_async_copy(hidden_part(me, h), cot.at[h, aligned(me, rows), :], local_sem.at[1]))
        for s, w in enumerate((w_gate, w_up)):
            mine.append(pltpu.make_async_copy(w.at[:, pl.ds(h * width, width)], held.at[h, s], local_sem.at[2]))
    pl.when(even)(lambda: mine[0].start())

    with jax.named_scope("barrier"):
        expected = nx + 1 + jnp.where(z >= 1, 1, 0) + jnp.where(z + 1 < nz, 1, 0)
        pl.semaphore_wait(barrier, jnp.where(odd, 1, expected))

    def remote(src, dst, send, recv, **to):
        return pltpu.make_async_remote_copy(
            src_ref=src, dst_ref=dst, send_sem=send, recv_sem=recv, device_id=to, device_id_type=MESH
        )

    def early(k, src, dst):
        return remote(src, dst, early_sems[0].at[k], early_sems[1].at[k], grp=far_grp)

    def start_early():
        place = aligned(me, rows)
        early(0, tokens, far_tok.at[place, :]).start()
        for s, w in enumerate((w_gate, w_up)):
            early(1, w.at[:, :width], far.at[0, s]).start()
        for j in range(1, n):
            to = lax.rem(me + j, n)
            early(2, hidden_part(to, 0), stage.at[:, aligned(to, width)]).start()
        early(2, hidden_part(me, 0), far_cot.at[0, aligned(me, rows), :]).start()

    def early_whole():
        return [early(k, ref, ref) for k, ref in enumerate((far_tok.at[aligned(me, rows), :], far.at[0], stage))]

    def relay(buf, sems):
        along_send, along_recv, side_send, side_recv = sems
        piece = rows // PIECES

        def slot(zz, xx, c):
            return buf.at[aligned((zz * nx + xx) * PIECES + c, piece), :]

        def along(zz, c, to):
            place = slot(zz, x, c)
            return remote(place, place, along_send, along_recv.at[zz, c], dp=to * nx + x)

        def up(zz, c, back=False):
            return along(zz, c, z - 1 if back else z + 1)

        def down(zz, c, back=False):
            return along(zz, c, z + 1 if back else z - 1)

        def side(zz, j, c):
            place = slot(zz, x, c)
            return remote(place, place, side_send, side_recv.at[zz, j - 1], dp=z * nx + lax.rem(x + j, nx))

        def pass_on(zz, c, upward):
            if upward is not False:
                pl.when(z + 1 < nz)(lambda: up(zz, c).start())
            if upward is not True:
                pl.when(z >= 1)(lambda: down(zz, c).start())
            for j in range(1, nx):
                side(zz, j, c).start()

        def begin():
            for c in range(PIECES):
                pass_on(z, c, None)

        def turn(r, then):
            for c in range(PIECES):
                @pl.when(z - 1 - r >= 0)
                def _():
                    with jax.named_scope("wait_up"):
                        up(z - 1 - r, c, True).wait_recv()
                    pass_on(z - 1 - r, c, True)

                @pl.when(z + 1 + r < nz)
                def _():
                    with jax.named_scope("wait_down"):
                        down(z + 1 + r, c, True).wait_recv()
                    pass_on(z + 1 + r, c, False)

            pl.when(z - 1 - r >= 0)(lambda: then(z - 1 - r))
            pl.when(z + 1 + r < nz)(lambda: then(z + 1 + r))

        def row_ready(zz):
            for j in range(1, nx):
                other = lax.rem(x + nx - j, nx)
                place = buf.at[aligned(zz * nx + other, rows), :]
                remote(place, place, side_send, side_recv.at[zz, j - 1], dp=z * nx + other).wait_recv()

        def settle():
            def sent(count, sem):
                place = buf.at[: count * rows, :]
                remote(place, place, sem, side_recv.at[0, 0], dp=lax.rem(me + 1, n)).wait_send()

            if nx > 1:
                sent(nz * (nx - 1), side_send)
            for at in range(nz):
                count = (at + 1 if at + 1 < nz else 0) + (nz - at if at >= 1 else 0)
                if count > 0:
                    pl.when(z == at)(lambda count=count: sent(count, along_send))

        return begin, turn, row_ready, settle

    def swap(block_of, buf, sems):
        def send_row(zz, h):
            for xx in range(nx):
                to = zz * nx + xx

                @pl.when(to != me)
                def _():
                    remote(
                        block_of(to, h), buf.at[h, aligned(me, rows), :], sems[0].at[0], sems[1].at[h], dp=to
                    ).start()

        def ready(h):
            place = buf.at[h, : (n - 1) * rows, :]
            remote(place, place, sems[0].at[0], sems[1].at[h], dp=lax.rem(me + 1, n)).wait_recv()

        def settle():
            place = buf.at[:, : (n - 1) * rows, :]
            remote(place, place, sems[0].at[0], sems[1].at[0], dp=lax.rem(me + 1, n)).wait_send()

        return send_row, ready, settle

    least = jnp.minimum(z, nz - 1 - z)
    longer = jnp.where(z < nz - 1 - z, 1, -1)

    def arriving(r):
        near_turn = r <= 2 * least
        step = jnp.where(near_turn, (r + 1) // 2, r - least)
        sign = jnp.where(near_turn, jnp.where(lax.rem(r, 2) == 1, -1, 1), longer)
        return z + sign * step

    def turn_over(buf, turned, zz):
        turned[:, aligned(zz, span)] = buf[aligned(zz, span), :].T

    def project(buf, gate_weight, up_weight, zz):
        part = aligned(zz, span)
        block = buf[part, :]
        gate_pre[part, :] = jnp.dot(block, gate_weight, preferred_element_type=F32) * scale
        up_pre[part, :] = jnp.dot(block, up_weight, preferred_element_type=F32) * scale

    def activate(cotangent, zz):
        part = aligned(zz, span)
        gate = gate_pre[part, :]
        sigma = jax.nn.sigmoid(gate)
        upstream = cotangent[part, :].astype(F32)
        gate_rows[part, :] = (upstream * up_pre[part, :] * sigma * (1.0 + gate * (1.0 - sigma))).astype(BF16)
        up_rows[part, :] = (upstream * gate * sigma).astype(BF16)

    def update(turned, weight, h, i):
        part = aligned(i, BLOCK)
        block = turned[part, :]
        for s, unit_rows in enumerate((gate_rows, up_rows)):
            gradient = jnp.dot(block, unit_rows[...], preferred_element_type=F32) * scale
            weight[h, s, part, :] = (weight[h, s, part, :].astype(F32) - 0.5 * gradient).astype(BF16)

    def near_copy(h, i):
        place = (h, slice(None), aligned(i, BLOCK))
        return remote(held.at[place], near.at[place], near_sems[0].at[0], near_sems[1].at[h], grp=near_grp)

    def near_slab(h):
        return remote(held.at[h], near.at[h], near_sems[0].at[0], near_sems[1].at[h], grp=near_grp)

    def far_copy(h, i):
        place = (h, slice(None), aligned(i, BLOCK))
        k = jnp.where(h == slabs - 1, h + i, h)
        last = jnp.where(h == slabs - 1, 1, 0)
        return remote(held.at[place], far.at[place], far_sems[0].at[last], far_sems[1].at[k], grp=far_grp)

    def far_slab(h):
        return remote(held.at[h], far.at[h], far_sems[0].at[0], far_sems[1].at[h], grp=far_grp)

    def far_sent(k, place):
        remote(held.at[place], far.at[place], far_sems[0].at[k], far_sems[1].at[0], grp=far_grp).wait_send()

    kept = blocks // 2

    def send_steps(h, i):
        now = (h < slabs - 1) | (i < kept) | (odd & jnp.logical_not(second))
        pl.when(now & (even | (h > 0)))(lambda: far_copy(h, i).start())
        near_copy(h, i).start()

    @pl.when(odd)
    def _():
        start_early()
        mine[0].start()
        with jax.named_scope("wait_turn"):
            pl.semaphore_wait(turn_sem, 1)

    begin, turn, tokens_ready, settle_tokens = relay(tok, gather_sems)
    send_cot, cot_ready, settle_cot = swap(hidden_part, cot, cot_sems)
    wait_mine(0)
    begin()
    for copy in mine[1:]:
        copy.start()
    send_cot(z, 0)
    wait_mine(1)
    wait_mine(2)

    @pl.loop(0, nz)
    def _(r):
        pl.when(r < nz - 1)(lambda: turn(r, lambda zz: send_cot(zz, 0)))
        zz = arriving(r)
        with jax.named_scope("wait_side"):
            tokens_ready(zz)
        with jax.named_scope("project"):
            turn_over(tok, tok_t, zz)
            project(tok, held[0, 0], held[0, 1], zz)

    @pl.loop(1, slabs)
    def _(h):
        @pl.loop(0, nz)
        def _(r):
            send_cot(arriving(r), h)

    @pl.loop(0, slabs)
    def _(h):
        @pl.when(h > 0)
        def _():
            @pl.loop(0, nz)
            def _(zz):
                project(tok, held[h, 0], held[h, 1], zz)

        with jax.named_scope("wait_cot"):
            cot_ready(h)

        @pl.loop(0, nz)
        def _(zz):
            with jax.named_scope("forward"):
                activate(cot.at[h], zz)

        @pl.when((h == slabs - 1) & even)
        def _():
            pl.semaphore_signal(turn_sem, inc=1, device_id={"grp": near_grp}, device_id_type=MESH)

        @pl.loop(0, blocks)
        def _(i):
            with jax.named_scope("step"):
                update(tok_t, held, h, i)
            pl.when(i >= 1)(lambda: send_steps(h, i - 1))

        send_steps(h, blocks - 1)

    settle_tokens()
    settle_cot()

    @pl.when(even)
    def _():
        with jax.named_scope("wait_sibling"):
            near_slab(0).wait_recv()
        for copy in early_whole():
            copy.wait_recv()
        begin, turn, tokens_ready, settle_far_tokens = relay(far_tok, gather_sems)
        send_cot, cot_ready, settle_far_cot = swap(
            lambda to, h: stage.at[:, aligned(to, width)], far_cot, cot_sems
        )
        begin()

        @pl.loop(0, nz)
        def _(r):
            send_cot(arriving(r), 0)

        @pl.loop(0, nz)
        def _(r):
            pl.when(r < nz - 1)(lambda: turn(r, lambda zz: None))
            zz = arriving(r)
            with jax.named_scope("wait_side"):
                tokens_ready(zz)
            with jax.named_scope("forward_far"):
                turn_over(far_tok, far_tok_t, zz)
                project(far_tok, far[0, 0], far[0, 1], zz)

        with jax.named_scope("wait_cot"):
            cot_ready(0)

        @pl.loop(0, nz)
        def _(zz):
            activate(far_cot.at[0], zz)

        @pl.loop(0, blocks)
        def _(i):
            with jax.named_scope("step_far"):
                update(far_tok_t, far, 0, i)

        settle_far_tokens()
        settle_far_cot()

    @pl.when(odd)
    def _():
        for copy in early_whole():
            copy.wait_send()

    @pl.loop(0, slabs)
    def _(h):
        with jax.named_scope("wait_near"):
            pl.when(odd | (h > 0))(lambda: near_slab(h).wait_recv())
        pl.when((h < slabs - 1) & (odd | (h > 0)))(lambda: far_slab(h).wait_recv())

        @pl.when(h == slabs - 1)
        def _():
            remote(held, near, near_sems[0].at[0], near_sems[1].at[0], grp=near_grp).wait_send()

        @pl.loop(0, jnp.where(second & (h == slabs - 1), kept, blocks))
        def _(i):
            with jax.named_scope("wait_far"):
                pl.when(h == slabs - 1)(lambda: far_copy(h, i).wait_recv())
            freed = i + kept - LAG
            behind = even & jnp.logical_not(second) & (h == slabs - 1)
            pl.when(behind & (freed >= kept) & (freed < blocks))(lambda: far_copy(h, freed).start())
            with jax.named_scope("mix"):
                part = aligned(i, BLOCK)
                for s in range(2):
                    far[h, s, part, :] = blend(held[h, s, part, :], near[h, s, part, :], far[h, s, part, :])

    pl.when(odd)(lambda: far_sent(0, pl.ds(1, slabs - 2)))
    pl.when(even)(lambda: far_sent(0, pl.ds(0, slabs - 1)))
    pl.when(second)(lambda: far_sent(1, (slabs - 1, slice(None), pl.ds(0, kept * BLOCK))))
    pl.when(jnp.logical_not(second))(lambda: far_sent(1, slabs - 1))


def closing_kernel(groups, mixed, held, near, placed, tail, send_sem, recv_sem):
    _, _, far_grp, second = roles(groups)
    last = held.shape[0] - 1
    depth = tail.shape[1]
    start = held.shape[2] - depth

    @pl.when(second)
    def _():
        barrier = pltpu.get_barrier_semaphore()
        pl.semaphore_signal(barrier, inc=1, device_id={"grp": far_grp}, device_id_type=MESH)
        pl.semaphore_wait(barrier, 1)

        def copy(i):
            return pltpu.make_async_remote_copy(
                src_ref=held.at[last, :, pl.ds(pl.multiple_of(start + i * BLOCK, BLOCK), BLOCK)],
                dst_ref=tail.at[:, aligned(i, BLOCK)], send_sem=send_sem.at[0], recv_sem=recv_sem.at[i],
                device_id={"grp": far_grp}, device_id_type=MESH,
            )

        @pl.loop(0, depth // BLOCK)
        def _(i):
            copy(i).start()

        @pl.loop(0, depth // BLOCK)
        def _(i):
            with jax.named_scope("wait_tail"):
                copy(i).wait_recv()
            part = aligned(i, BLOCK)
            rows = pl.ds(pl.multiple_of(start + i * BLOCK, BLOCK), BLOCK)
            for s in range(2):
                tail[s, part, :] = blend(held[last, s, rows, :], near[last, s, rows, :], tail[s, part, :])

        pltpu.make_async_remote_copy(
            src_ref=tail, dst_ref=tail, send_sem=send_sem.at[0], recv_sem=recv_sem.at[0],
            device_id={"grp": far_grp}, device_id_type=MESH,
        ).wait_send()

    @pl.when(jnp.logical_not(second))
    def _():
        for s in range(2):
            tail[s] = mixed[last, s, start:, :]


def place_kernel(mixed, out_gate, out_up, sems):
    slabs, _, depth, width = mixed.shape
    copies = []
    for h in range(slabs):
        step = depth // 4
        for start in range(0, depth if h < slabs - 1 else depth - closing_rows(depth), step):
            for s, out in enumerate((out_gate, out_up)):
                rows = pl.ds(start, step)
                copies.append(
                    pltpu.make_async_copy(mixed.at[h, s, rows], out.at[rows, pl.ds(h * width, width)], sems.at[len(copies)])
                )
    for copy in copies:
        copy.start()
    for copy in copies:
        copy.wait()


def place_tail_kernel(tail, held_gate, held_up, out_gate, out_up, sems):
    _, rows, width = tail.shape
    depth, units = out_gate.shape
    step = rows // 2
    copies = [
        pltpu.make_async_copy(
            tail.at[s, pl.ds(k * step, step)],
            out.at[pl.ds(depth - rows + k * step, step), pl.ds(units - width, width)], sems.at[s, k],
        )
        for s, out in enumerate((out_gate, out_up))
        for k in range(2)
    ]
    for copy in copies:
        copy.start()
    for copy in copies:
        copy.wait()


def local(tokens, hidden_grad, w_gate, w_up):
    n, groups = lax.axis_size("dp"), lax.axis_size("grp")
    nx = inner_size(n)
    nz = n // nx
    args = [pltpu.with_memory_space_constraint(a[0], pltpu.HBM) for a in (tokens, hidden_grad, w_gate, w_up)]
    rows, depth = args[0].shape
    units = args[2].shape[1]
    total = n * rows
    slabs = slab_count(units)
    width = units // slabs
    blocks = depth // BLOCK
    dma = pltpu.SemaphoreType.DMA
    hops = [dma, dma((nz, PIECES)), dma, dma((nz, max(nx - 1, 1)))]
    weights = (slabs, 2, depth, width)
    scratch = [
        pltpu.VMEM((total, depth), BF16),
        pltpu.VMEM((depth, total), BF16),
        pltpu.VMEM((slabs, total, width), BF16),
        pltpu.VMEM((total, depth), BF16),
        pltpu.VMEM((depth, total), BF16),
        pltpu.VMEM((1, total, width), BF16),
        pltpu.VMEM((rows, n * width), BF16),
        pltpu.VMEM((total, width), BF16),
        pltpu.VMEM((total, width), BF16),
        pltpu.VMEM((total, width), F32),
        pltpu.VMEM((total, width), F32),
        dma((3,)), pltpu.SemaphoreType.REGULAR,
        *hops,
        dma((1,)), dma((slabs,)),
        dma((3,)), dma((3,)),
        dma((1,)), dma((slabs,)),
        dma((2,)), dma((slabs - 1 + blocks,)),
    ]
    kept = pltpu.VMEM(weights, BF16)
    mixed, held, near = pl.pallas_call(
        functools.partial(kernel, n, groups),
        out_shape=[kept, kept, kept],
        in_specs=[ANY] * 4,
        out_specs=[VMEM] * 3,
        scratch_shapes=scratch,
        compiler_params=pltpu.CompilerParams(
            collective_id=0, has_side_effects=True, vmem_limit_bytes=VMEM_LIMIT
        ),
        name="gossip_step",
    )(*args)
    mixed, held, near = (pltpu.with_memory_space_constraint(a, pltpu.VMEM) for a in (mixed, held, near))
    shape = jax.ShapeDtypeStruct((depth, units), BF16)
    outs = pl.pallas_call(
        place_kernel,
        out_shape=[shape, shape],
        in_specs=[VMEM],
        out_specs=[ANY] * 2,
        scratch_shapes=[dma((8 * slabs,))],
        compiler_params=pltpu.CompilerParams(vmem_limit_bytes=SMALL_LIMIT),
        name="place",
    )(mixed)
    tail_rows = closing_rows(depth)
    tail = pl.pallas_call(
        functools.partial(closing_kernel, groups),
        out_shape=pltpu.VMEM((2, tail_rows, width), BF16),
        in_specs=[VMEM] * 3 + [ANY],
        out_specs=VMEM,
        scratch_shapes=[dma((1,)), dma((tail_rows // BLOCK,))],
        compiler_params=pltpu.CompilerParams(
            collective_id=1, has_side_effects=True, vmem_limit_bytes=SMALL_LIMIT
        ),
        name="closing",
    )(mixed, held, near, pltpu.with_memory_space_constraint(outs[0], pltpu.HBM))
    outs = pl.pallas_call(
        place_tail_kernel,
        out_shape=[shape, shape],
        in_specs=[VMEM, ANY, ANY],
        out_specs=[ANY] * 2,
        input_output_aliases={1: 0, 2: 1},
        scratch_shapes=[dma((2, 2))],
        compiler_params=pltpu.CompilerParams(vmem_limit_bytes=SMALL_LIMIT),
        name="place_tail",
    )(
        pltpu.with_memory_space_constraint(tail, pltpu.VMEM),
        *(pltpu.with_memory_space_constraint(out, pltpu.HBM) for out in outs),
    )
    return tuple(out[None] for out in outs)


def solution(mesh):
    in_specs = (
        P("grp", "dp", None),
        P("grp", "dp", None),
        P("grp", None, "dp"),
        P("grp", None, "dp"),
    )
    out_specs = (P("grp", None, "dp"), P("grp", None, "dp"))
    return jax.shard_map(local, mesh=mesh, in_specs=in_specs, out_specs=out_specs, check_vma=False)
```
